32 devices in a mesh: section: 2 (over x), slab: 16 (over z, y, core).
Axes of the slice: x: 2, y: 2, z: 4, core: 2. Of those that a mesh axis runs over, the one named last changes fastest.
Arguments:
- concentration: float32 [4, 2048, 2048], P('section', 'slab'), may hold values from -3.2 to 3.2
Outputs:
- new_concentration: float32 [4, 2048, 2048], P('section', 'slab')
- energy: float32 [], replicated
The draws below stay inside these ranges and needn't reach their ends.
All inputs are finite; a program needn't handle non-finite values.
Results may differ from the reference program's by a relative error of at most 0.000098.
Values sent between devices are 32-bit elements; how exact they have to be, the bound alone decides.
A program may use at most 64 MiB of HBM per device.

```python
import math
import jax
import jax.numpy as jnp
from jax import lax

NX = 2048
NY = 2048
NZ = 4


def blur_weights(extent, coarse_total, blur_width):
    position = jnp.arange(extent, dtype=jnp.float32)
    spacing = extent / coarse_total
    centers = (jnp.arange(coarse_total, dtype=jnp.float32) + 0.5) * spacing
    offset = position[:, None] - centers[None, :]
    offset = jnp.mod(offset + 0.5 * extent, extent) - 0.5 * extent
    weights = jnp.exp(-offset * offset / (2.0 * blur_width * blur_width))
    return weights / jnp.sqrt(jnp.sum(weights * weights, axis=1, keepdims=True))


def draw_concentration(key, part):
    base_key = jax.random.fold_in(key, 7)
    noise_key = jax.random.fold_in(base_key, 0)
    smooth_key = jax.random.fold_in(base_key, 2)
    coarse_x = max(NX // 16, 4)
    coarse_y = max(NY // 16, 4)
    coarse = jax.random.normal(smooth_key, (NZ, coarse_x, coarse_y), jnp.float32)
    along_x = blur_weights(NX, coarse_x, 16.0)
    along_y = blur_weights(NY, coarse_y, 16.0)
    smooth = jnp.einsum('zij,xi->zxj', coarse, along_x, precision=lax.Precision.HIGHEST)
    smooth = jnp.einsum('zxj,yj->zxy', smooth, along_y, precision=lax.Precision.HIGHEST)
    depth_pos = jnp.arange(NZ, dtype=jnp.float32) / NZ
    row_pos = jnp.arange(NX, dtype=jnp.float32) / NX
    spread = 0.45 * (1.0 + 1.2 * row_pos[None, :, None] + 0.6 * depth_pos[:, None, None])
    jitter = jax.random.truncated_normal(noise_key, -2.5, 2.5, (NZ, NX, NY), jnp.float32)
    values = 0.6 * smooth + jitter * spread
    values = jnp.clip(values, -3.2, 3.2)
    return values.astype(jnp.float32)


def setup_inputs(seed: int = 0) -> dict:
    arg_keys = jax.random.split(jax.random.key(seed), 2)
    return {
        "concentration": draw_concentration(jax.random.fold_in(arg_keys[1], 71), 0),
    }


time_step = 100.0
kappa_grad = 2.0
stabilizer = 8.0


def wave_square(length):
    position = jnp.arange(length, dtype=jnp.int32)
    signed = jnp.where(2 * position >= length, position - length, position)
    phase_angle = signed.astype(jnp.float32) * (2.0 * math.pi / length)
    return phase_angle * phase_angle


def reference(concentration):
    squared = concentration * concentration
    bulk_sum = jnp.sum(0.25 * squared * squared - 0.5 * squared)
    cubic_term = squared * concentration - concentration
    spec_c = jnp.fft.fftn(concentration)
    spec_g = jnp.fft.fftn(cubic_term)
    wave_sq = wave_square(NZ)[:, None, None] + wave_square(NX)[None, :, None] + wave_square(NY)[None, None, :]
    numerator = 1.0 + time_step * stabilizer * wave_sq
    denominator = numerator + time_step * kappa_grad * wave_sq * wave_sq
    updated = (numerator * spec_c - time_step * wave_sq * spec_g) / denominator
    new_field = jnp.real(jnp.fft.ifftn(updated)).astype(jnp.float32)
    cell_count = NX * NY * NZ
    energy = (bulk_sum / cell_count).astype(jnp.float32)
    return (new_field, energy)
```

```python
import functools
import math

import jax
import jax.numpy as jnp
import numpy as np
from jax import lax
from jax.experimental import pallas as pl
from jax.experimental.pallas import tpu as pltpu
from jax.sharding import PartitionSpec as P

time_step = 100.0
kappa_grad = 2.0
stabilizer = 8.0
highest = lax.Precision.HIGHEST


def circle(length, first_total, second_total, direction):
    first_index = jnp.arange(first_total, dtype=jnp.int32)
    second_index = jnp.arange(second_total, dtype=jnp.int32)
    turn_index = first_index[:, None] * second_index[None, :] % length
    phase_angle = turn_index.astype(jnp.float32) * (2.0 * math.pi / length)
    return (jnp.cos(phase_angle), direction * jnp.sin(phase_angle))


def contract(pattern, real_part, imag_part, table_cos, table_sin):

    def product_of(operand, matrix):
        return jnp.einsum(pattern, operand, matrix, precision=highest)

    out_real = product_of(real_part, table_cos) - product_of(imag_part, table_sin)
    out_imag = product_of(real_part, table_sin) + product_of(imag_part, table_cos)
    return (out_real, out_imag)


def real_only(pattern, real_part, imag_part, table_cos, table_sin):
    return jnp.einsum(pattern, real_part, table_cos, precision=highest) - jnp.einsum(
        pattern, imag_part, table_sin, precision=highest
    )


def rotate(real_part, imag_part, table_cos, table_sin):
    return (
        real_part * table_cos - imag_part * table_sin,
        real_part * table_sin + imag_part * table_cos,
    )


def wave_square(storage, length, permuted):
    if permuted:
        actual = storage // 128 + length // 128 * (storage % 128)
    else:
        actual = storage
    signed = jnp.where(2 * actual >= length, actual - length, actual)
    phase_angle = signed.astype(jnp.float32) * (2.0 * math.pi / length)
    return phase_angle * phase_angle


def plain_step(concentration):
    plane_count, row_count, full_y = concentration.shape
    slab_count = lax.axis_size("slab")
    section_count = lax.axis_size("section")
    full_x = row_count * slab_count
    full_z = plane_count * section_count
    y_block = full_y // slab_count
    y_half = y_block // section_count
    blocks_x = full_x // 128
    blocks_y = full_y // 128
    cell_count = full_x * full_y * full_z
    slab_at = lax.axis_index("slab")
    section_at = lax.axis_index("section")
    squared = concentration * concentration
    bulk_sum = jnp.sum(0.25 * squared * squared - 0.5 * squared)
    cubic_term = squared * concentration - concentration
    shaped_c = concentration.reshape(1, plane_count, row_count, blocks_y, 128)
    shaped_g = cubic_term.reshape(1, plane_count, row_count, blocks_y, 128)
    first_cos, first_sin = circle(blocks_y, blocks_y, blocks_y, -1.0)
    part_real, part_imag = contract("fzxab,aj->fzxjb", shaped_c, shaped_g, first_cos, first_sin)
    field_total = part_real.shape[0]
    twist_cos, twist_sin = circle(full_y, blocks_y, 128, -1.0)
    part_real, part_imag = rotate(part_real, part_imag, twist_cos, twist_sin)
    lane_cos, lane_sin = circle(128, 128, 128, -1.0)
    part_real, part_imag = contract("fzxjb,bk->fxjkz", part_real, part_imag, lane_cos, lane_sin)
    outgoing = jnp.concatenate([part_real, part_imag], 0).reshape(
        2 * field_total, row_count, slab_count, y_block * plane_count
    )
    columns = lax.all_to_all(outgoing, "slab", split_axis=2, concat_axis=1, tiled=True)
    columns = columns.reshape(2 * field_total, blocks_x, 128, y_block * plane_count)
    first_cos, first_sin = circle(blocks_x, blocks_x, blocks_x, -1.0)
    part_real, part_imag = contract(
        "fabm,aj->fmjb", columns[:field_total], columns[field_total:], first_cos, first_sin
    )
    twist_cos, twist_sin = circle(full_x, blocks_x, 128, -1.0)
    part_real, part_imag = rotate(part_real, part_imag, twist_cos, twist_sin)
    part_real, part_imag = contract("fmjb,bk->fmjk", part_real, part_imag, lane_cos, lane_sin)
    spectra_x = jnp.concatenate([part_real, part_imag], 0).reshape(
        2 * field_total, y_block, plane_count, full_x
    )
    depth_cos, depth_sin = circle(full_z, full_z, full_z, -1.0)
    own_cos = lax.dynamic_slice_in_dim(depth_cos, section_at * plane_count, plane_count, 0)
    own_sin = lax.dynamic_slice_in_dim(depth_sin, section_at * plane_count, plane_count, 0)
    term_real, term_imag = contract(
        "fyzk,zq->yfqk", spectra_x[:field_total], spectra_x[field_total:], own_cos, own_sin
    )
    spectral = lax.psum_scatter(
        jnp.concatenate([term_real, term_imag], 1), "section", scatter_dimension=0, tiled=True
    )
    storage_y = slab_at * y_block + section_at * y_half + jnp.arange(y_half, dtype=jnp.int32)
    storage_x = jnp.arange(full_x, dtype=jnp.int32)
    storage_z = jnp.arange(full_z, dtype=jnp.int32)
    wave_sq = (
        wave_square(storage_y, full_y, True)[:, None, None]
        + wave_square(storage_z, full_z, False)[None, :, None]
        + wave_square(storage_x, full_x, True)[None, None, :]
    )
    numerator = 1.0 + time_step * stabilizer * wave_sq
    denominator = numerator + time_step * kappa_grad * wave_sq * wave_sq
    keep_rate = numerator / denominator
    mix_rate = time_step * wave_sq / denominator
    new_real = keep_rate * spectral[:, 0] - mix_rate * spectral[:, 1]
    new_imag = keep_rate * spectral[:, 1] + mix_rate * spectral[:, 0]
    back_cos, back_sin = circle(full_z, full_z, full_z, 1.0)
    part_real, part_imag = contract("yqk,qz->yzk", new_real, new_imag, back_cos, back_sin)
    returning = jnp.stack([part_real, part_imag], 1)
    own_planes = lax.all_to_all(returning, "section", split_axis=2, concat_axis=0, tiled=True)
    grid_real = own_planes[:, 0].reshape(y_block, plane_count, blocks_x, 128)
    grid_imag = own_planes[:, 1].reshape(y_block, plane_count, blocks_x, 128)
    lane_cos, lane_sin = circle(128, 128, 128, 1.0)
    part_real, part_imag = contract("szjk,kb->szjb", grid_real, grid_imag, lane_cos, lane_sin)
    twist_cos, twist_sin = circle(full_x, blocks_x, 128, 1.0)
    part_real, part_imag = rotate(part_real, part_imag, twist_cos, twist_sin)
    first_cos, first_sin = circle(blocks_x, blocks_x, blocks_x, 1.0)
    part_real, part_imag = contract("szjb,ja->absz", part_real, part_imag, first_cos, first_sin)
    leaving = jnp.stack([part_real, part_imag], 0).reshape(2, full_x, 1, y_block * plane_count)
    rows_back = lax.all_to_all(leaving, "slab", split_axis=1, concat_axis=2, tiled=True)
    rows_back = rows_back.reshape(2, row_count, blocks_y, 128, plane_count)
    part_real, part_imag = contract("xjkz,kb->xjbz", rows_back[0], rows_back[1], lane_cos, lane_sin)
    twist_cos, twist_sin = circle(full_y, blocks_y, 128, 1.0)
    part_real, part_imag = rotate(
        part_real, part_imag, twist_cos[:, :, None], twist_sin[:, :, None]
    )
    first_cos, first_sin = circle(blocks_y, blocks_y, blocks_y, 1.0)
    new_field = real_only("xjbz,ja->zxab", part_real, part_imag, first_cos, first_sin)
    new_field = new_field.reshape(plane_count, row_count, full_y) / cell_count
    total_bulk = lax.psum(bulk_sum, ("section", "slab"))
    energy = total_bulk / cell_count
    return (new_field, energy)


lanes = 128
row_group = 32
vmem_limit = 62 * 1024 * 1024


def split(values):
    high = values.astype(jnp.bfloat16)
    low = (values - high.astype(jnp.float32)).astype(jnp.bfloat16)
    return high, low


def triple(left_parts, right_parts, dims):
    def product(left, right):
        return lax.dot_general(left, right, (dims, ((), ())), preferred_element_type=jnp.float32)

    left_high, left_low = left_parts
    right_high, right_low = right_parts
    return (
        product(left_high, right_high)
        + product(left_low, right_high)
        + product(left_high, right_low)
    )


def y_tables(full_y, devices, parity):
    half = full_y // 2
    per_part = half // 2 // devices
    slot = np.arange(half)
    device, inner = slot // (2 * per_part), slot % (2 * per_part)
    part, local = inner // per_part, inner % per_part
    wave = parity + 2 * (device * per_part + local)
    position = np.arange(half)
    turns = wave[:, None] * position[None, :] % full_y
    phase = turns * (2.0 * math.pi / full_y)
    coarse = phase[::row_group]
    offset = wave[:row_group] - wave[0]
    fine = (offset[:, None] * position[None, :] % full_y) * (2.0 * math.pi / full_y)
    fine = fine + part[:row_group, None] * (0.5 * math.pi)
    return [
        table.astype(np.float32)
        for table in (np.cos(coarse), np.sin(coarse), np.cos(fine), np.sin(fine))
    ]


def y_block(refs, block, groups, parity):
    coarse_cos, coarse_sin, fine_cos, fine_sin = refs
    cos_fine, sin_fine = fine_cos[...], fine_sin[...]
    pieces = []
    for inner in range(groups):
        at = pl.ds(block * groups + inner, 1)
        piece = coarse_cos[at, :] * cos_fine - coarse_sin[at, :] * sin_fine
        if parity == 0 and inner == 0:
            row = lax.broadcasted_iota(jnp.int32, piece.shape, 0)
            column = lax.broadcasted_iota(jnp.int32, piece.shape, 1)
            sign = 1.0 - 2.0 * (column % 2).astype(jnp.float32)
            wanted = jnp.where(block == 0, row_group // 2, -1)
            piece = jnp.where(row == wanted, sign, piece)
        pieces.append(piece)
    return jnp.concatenate(pieces, 0)


def times_unit(real, imag, quarter_turns):
    turns = quarter_turns % 4
    if turns == 0:
        return real, imag
    if turns == 1:
        return -imag, real
    if turns == 2:
        return -real, -imag
    return imag, -real


def unit_sum(parts, power, direction):
    total_real, total_imag = parts[0]
    for index in range(1, len(parts)):
        real, imag = times_unit(*parts[index], direction * power * index)
        total_real = total_real + real
        total_imag = total_imag + imag
    return total_real, total_imag


groups = 8
chunks = 4


def flip(bit, wanted):
    return 1 - bit if wanted else bit


class Place:
    def __init__(self):
        self.section = lax.axis_index("section")
        self.slab = lax.axis_index("slab")
        self.upper = self.slab // 8
        self.bits = [self.slab % 2, self.slab // 2 % 2, self.slab // 4 % 2, self.section]
        self.member = self.index_of(self.bits)

    @staticmethod
    def index_of(bits):
        return bits[3] * 8 + bits[2] * 4 + bits[1] * 2 + bits[0]

    def peer(self, turn):
        bits = [flip(bit, turn >> at & 1) for at, bit in enumerate(self.bits)]
        slab = self.upper * 8 + bits[2] * 4 + bits[1] * 2 + bits[0]
        return self.index_of(bits), (bits[3], slab)

    def partner(self):
        return self.section, (1 - self.upper) * 8 + self.slab % 8


def remote(source, target, send, receive, device):
    return pltpu.make_async_remote_copy(
        src_ref=source,
        dst_ref=target,
        send_sem=send,
        recv_sem=receive,
        device_id=device,
        device_id_type=pl.DeviceIdType.MESH,
    )


turn_order = list(range(1, 16))


def greet(place):
    barrier = pltpu.get_barrier_semaphore()
    devices = [place.peer(turn)[1] for turn in turn_order] + [place.partner()]
    for device in devices:
        pl.semaphore_signal(
            barrier, inc=1, device_id=device, device_id_type=pl.DeviceIdType.MESH
        )
    pl.semaphore_wait(barrier, len(devices))


def step_kernel(cells, conc_ref, *refs):
    tables = [refs[0:4], refs[4:8]]
    wx_ref, tw_cos, tw_sin, ca, sa, cb, sb = refs[8:15]
    out_ref, energy_ref = refs[15:17]
    (
        high_ref, low_ref, wide_high, wide_low, spec_ref, fil_ref, back_ref, even_ref,
        sent_ref, arrived_ref, own_ref, other_ref, partner_ref, returned_ref,
        tile_ref, half_ref, far_ref,
        sent_out, sent_in, other_out, other_in, own_out, own_in, tile_out, tile_in,
        half_out, half_in,
    ) = refs[17:]
    place = Place()
    member = place.member
    planes, rows, full_y = conc_ref.shape
    half = full_y // 2
    members, inner, columns = arrived_ref.shape[1:]
    kk = inner // 2
    width = spec_ref.shape[4]
    padded = kk + 8
    sections = 2
    full_z = planes * sections
    zf_local = planes * 2
    total_zf = zf_local * sections
    slabs = members // sections
    quarter = slabs // 2
    greet(place)

    def prepare(parity):
        total = jnp.zeros((8, lanes), jnp.float32)
        for plane in range(planes):
            first = conc_ref[plane, :, :half]
            second = conc_ref[plane, :, half:]
            first_sq, second_sq = first * first, second * second
            if parity == 0:
                bulk = 0.25 * (first_sq * first_sq + second_sq * second_sq)
                bulk = bulk - 0.5 * (first_sq + second_sq)
                bulk = jnp.sum(bulk.reshape(rows // 8, 8, half), axis=0)
                for at in range(0, half, lanes):
                    total = total + bulk[:, at : at + lanes]
            first_g = first_sq * first - first
            second_g = second_sq * second - second
            for field, (left, right) in enumerate(((first, second), (first_g, second_g))):
                mixed = left + right if parity == 0 else left - right
                high, low = split(mixed)
                at = (plane * 2 + field) * rows
                high_ref[at : at + rows, :] = high
                low_ref[at : at + rows, :] = low
        return total

    def forward(chunk):
        parity, sub = chunk // 2, chunk % 2
        blocks = members // groups

        def one(block, carry):
            table = y_block(tables[parity], sub * blocks + block, groups, parity)
            result = triple(split(table), (high_ref[...], low_ref[...]), ((1,), (1,)))
            sent_ref[chunk, pl.ds(block * groups, groups)] = result.reshape(groups, inner, columns)
            return carry

        lax.fori_loop(0, blocks, one, 0)
        arrived_ref[chunk, member] = sent_ref[chunk, member]

    def spread(chunk):
        copies = []
        for turn in turn_order:
            peer, device = place.peer(turn)
            copies.append(
                remote(
                    sent_ref.at[chunk, peer],
                    arrived_ref.at[chunk, member],
                    sent_out.at[chunk, turn],
                    sent_in.at[chunk, turn],
                    device,
                )
            )
        for copy in copies:
            copy.start()
        return copies

    def spread_tile():
        copies = []
        for turn in turn_order:
            copies.append(
                remote(
                    tile_ref.at[member],
                    tile_ref.at[member],
                    tile_out.at[turn],
                    tile_in.at[turn],
                    place.peer(turn)[1],
                )
            )
        for copy in copies:
            copy.start()
        return copies

    def middle(chunk):
        parity, sub = chunk // 2, chunk % 2
        has_extra = chunk == 0
        depth = padded if has_extra else kk
        base_wave = parity + 2 * kk * (sub * members + member)
        row_iota = lax.broadcasted_iota(jnp.int32, (8, 1), 0)
        special = None
        if has_extra:
            wanted = jnp.where(member == 0, 0, -1)
            special = jnp.where(row_iota == wanted, 1.0, 0.0)

        def gather(section, a, part, row, zf):
            pieces = [
                arrived_ref[
                    chunk,
                    section * slabs + a * quarter + step,
                    part * kk + row : part * kk + row + 8,
                    zf * lanes : (zf + 1) * lanes,
                ]
                for step in range(quarter)
            ]
            return jnp.concatenate(pieces, 1)

        for section in range(sections):
            for zf in range(zf_local):
                at = section * zf_local + zf
                for row in range(0, depth, 8):
                    source = 0 if row >= kk else row
                    parts = []
                    for a in range(2):
                        imag = gather(section, a, 1, source, zf)
                        if row >= kk:
                            real, imag = imag * special, jnp.zeros_like(imag)
                        else:
                            real = gather(section, a, 0, source, zf)
                            if has_extra and row == 0:
                                imag = imag * (1.0 - special)
                        parts.append((real, imag))
                    for j in range(4):
                        real, imag = unit_sum(parts, j, -1)
                        if j:
                            cos, sin = tw_cos[j : j + 1, :], tw_sin[j : j + 1, :]
                            real, imag = real * cos + imag * sin, imag * cos - real * sin
                        spec_ref[j, 0, at, row : row + 8, :] = real
                        spec_ref[j, 1, at, row : row + 8, :] = imag

        def one(j, carry):
            source = spec_ref[j, :, :, 0:depth, :].reshape(2 * total_zf * depth, width)
            weights = (wide_high[...], wide_low[...])
            raw = triple(split(source), weights, ((1,), (0,)))
            raw = raw.reshape(2, total_zf, depth, 2 * width)
            for row in range(0, depth, 8):
                fields = []
                for field in range(2):
                    per_z = []
                    for z in range(full_z):
                        at = z * 2 + field
                        re_part = raw[0, at, row : row + 8]
                        im_part = raw[1, at, row : row + 8]
                        per_z.append(
                            (
                                re_part[:, :width] + im_part[:, width:],
                                im_part[:, :width] - re_part[:, width:],
                            )
                        )
                    fields.append(per_z)
                wave = base_wave + 2 * (row + row_iota)
                if row >= kk:
                    wave = jnp.full_like(wave, half)
                first = (wave == 0) | (wave == half)
                weight = jnp.where(first, 1.0 / cells, 2.0 / cells)
                angle = wave.astype(jnp.float32) * (2.0 * math.pi / full_y)
                plane_sq = angle * angle + wx_ref[pl.ds(j, 1), :]
                updated = []
                for q in range(full_z):
                    c_real, c_imag = unit_sum(fields[0], q, -1)
                    g_real, g_imag = unit_sum(fields[1], q, -1)
                    signed = q - full_z if 2 * q >= full_z else q
                    wave_sq = plane_sq + (2.0 * math.pi * signed / full_z) ** 2
                    numerator = 1.0 + time_step * stabilizer * wave_sq
                    denominator = numerator + time_step * kappa_grad * wave_sq * wave_sq
                    inverse = weight / denominator
                    keep = numerator * inverse
                    mix = time_step * wave_sq * inverse
                    updated.append((keep * c_real - mix * g_real, keep * c_imag - mix * g_imag))
                for z in range(full_z):
                    real, imag = unit_sum(updated, z, 1)
                    fil_ref[0, z, row : row + 8, :] = real
                    fil_ref[1, z, row : row + 8, :] = imag
            source = fil_ref[:, :, 0:depth, :].reshape(2 * full_z * depth, width)
            raw = triple(split(source), weights, ((1,), (0,)))
            raw = raw.reshape(2, full_z, depth, 2 * width)
            real = raw[0, :, :, :width] - raw[1, :, :, width:]
            imag = raw[0, :, :, width:] + raw[1, :, :, :width]
            cos, sin = tw_cos[pl.ds(j, 1), :], tw_sin[pl.ds(j, 1), :]
            back_ref[j, 0, :, 0:depth, :] = real * cos - imag * sin
            back_ref[j, 1, :, 0:depth, :] = imag * cos + real * sin
            return carry

        lax.fori_loop(0, 4, one, 0)
        for z in range(full_z):
            section, plane = z // planes, z % planes
            for row in range(0, kk, 8):
                parts = [
                    (back_ref[j, 0, z, row : row + 8, :], back_ref[j, 1, z, row : row + 8, :])
                    for j in range(4)
                ]
                extra = None
                if has_extra and row == 0:
                    extra = [
                        (back_ref[j, 0, z, kk : kk + 8, :], back_ref[j, 1, z, kk : kk + 8, :])
                        for j in range(4)
                    ]
                for a in range(4):
                    real, imag = unit_sum(parts, a, 1)
                    if extra is not None:
                        extra_real, _ = unit_sum(extra, a, 1)
                        imag = imag * (1.0 - special) + extra_real * special
                    target_ref = own_ref if a < 2 else other_ref
                    for step in range(quarter):
                        target = section * slabs + a % 2 * quarter + step
                        piece = slice(step * lanes, (step + 1) * lanes)
                        at = plane * inner + row
                        target_ref[chunk, target, at : at + 8, :] = real[:, piece]
                        target_ref[chunk, target, at + kk : at + kk + 8, :] = imag[:, piece]

    def cross(chunk):
        copy = remote(
            other_ref.at[chunk],
            partner_ref.at[chunk],
            other_out.at[chunk],
            other_in.at[chunk],
            place.partner(),
        )
        copy.start()
        return copy

    def join(chunk):
        own_ref[chunk] = own_ref[chunk] + partner_ref[chunk]
        returned_ref[chunk, member] = own_ref[chunk, member]

    def give_back(chunk):
        copies = []
        for turn in turn_order:
            peer, device = place.peer(turn)
            copies.append(
                remote(
                    own_ref.at[chunk, peer],
                    returned_ref.at[chunk, member],
                    own_out.at[chunk, turn],
                    own_in.at[chunk, turn],
                    device,
                )
            )
        for copy in copies:
            copy.start()
        return copies

    def backward(chunk):
        parity, sub = chunk // 2, chunk % 2
        blocks = members // groups
        total = None
        for block in range(blocks):
            at = slice(block * groups, (block + 1) * groups)
            turned = [
                returned_ref[chunk, at, plane * inner : (plane + 1) * inner, :]
                .reshape(groups * inner, rows)
                .T
                for plane in range(planes)
            ]
            table = y_block(tables[parity], sub * blocks + block, groups, parity)
            term = triple(split(jnp.concatenate(turned, 0)), split(table), ((1,), (0,)))
            total = term if total is None else total + term
        return total

    def wait_in(copies):
        for copy in copies:
            copy.wait_recv()

    tile_ref[member] = prepare(0)
    forward(0)
    spreads = {0: spread(0)}
    tiles = spread_tile()
    forward(1)
    spreads[1] = spread(1)
    cos_rows, sin_rows = [], []
    cos_fine, sin_fine = cb[...], sb[...]
    for group in range(ca.shape[0]):
        cos_base, sin_base = ca[group : group + 1, :], sa[group : group + 1, :]
        cos_rows.append(cos_base * cos_fine - sin_base * sin_fine)
        sin_rows.append(sin_base * cos_fine + cos_base * sin_fine)
    table = jnp.concatenate([jnp.concatenate(cos_rows, 0), jnp.concatenate(sin_rows, 0)], 1)
    wide_high[...], wide_low[...] = split(table)
    prepare(1)
    forward(2)
    forward(3)
    crosses = {}
    backs = {}
    wait_in(spreads[0])
    middle(0)
    crosses[0] = cross(0)
    spreads[2] = spread(2)
    wait_in(tiles)
    half_ref[...] = jnp.sum(tile_ref[...], axis=0)
    far = remote(half_ref, far_ref, half_out, half_in, place.partner())
    far.start()
    wait_in(spreads[1])
    middle(1)
    crosses[1] = cross(1)
    spreads[3] = spread(3)
    wait_in(spreads[2])
    middle(2)
    crosses[2] = cross(2)
    crosses[0].wait_recv()
    join(0)
    backs[0] = give_back(0)
    wait_in(spreads[3])
    middle(3)
    crosses[3] = cross(3)
    crosses[1].wait_recv()
    join(1)
    backs[1] = give_back(1)
    crosses[2].wait_recv()
    join(2)
    backs[2] = give_back(2)
    wait_in(backs[0])
    even_ref[...] = backward(0)
    wait_in(backs[1])
    even_ref[...] = even_ref[...] + backward(1)
    crosses[3].wait_recv()
    join(3)
    backs[3] = give_back(3)
    wait_in(backs[2])
    odd = backward(2)
    wait_in(backs[3])
    odd = odd + backward(3)
    for plane in range(planes):
        even_rows = even_ref[plane * rows : (plane + 1) * rows, :]
        odd_rows = odd[plane * rows : (plane + 1) * rows, :]
        out_ref[plane, :, :half] = even_rows + odd_rows
        out_ref[plane, :, half:] = even_rows - odd_rows
    far.wait_recv()
    energy_ref[0, 0] = jnp.sum(half_ref[...] + far_ref[...]) / cells
    for chunk in range(chunks):
        for copy in spreads[chunk] + backs[chunk] + [crosses[chunk]]:
            copy.wait_send()
    for copy in tiles + [far]:
        copy.wait_send()


def kernel_step(concentration):
    planes, rows, full_y = concentration.shape
    slabs = lax.axis_size("slab")
    sections = lax.axis_size("section")
    devices = slabs * sections
    members = devices // 2
    full_x = rows * slabs
    full_z = planes * sections
    cells = full_x * full_y * full_z
    half = full_y // 2
    kk = half // 2 // devices
    width = full_x // 4
    base = np.arange(width)
    step = 2.0 * math.pi / width
    coarse = base[::row_group, None] * base[None, :] % width * step
    fine = base[:row_group, None] * base[None, :] % width * step
    dft = [f(t).astype(np.float32) for t in (coarse, fine) for f in (np.cos, np.sin)]
    twist = np.arange(4)[:, None] * base[None, :] * (2.0 * math.pi / full_x)
    twist_cos, twist_sin = np.cos(twist).astype(np.float32), np.sin(twist).astype(np.float32)
    kx = np.arange(4)[:, None] + 4 * base[None, :]
    kx = np.where(2 * kx >= full_x, kx - full_x, kx) * (2.0 * math.pi / full_x)
    wave_x = (kx * kx).astype(np.float32)
    tables = [y_tables(full_y, devices, parity) for parity in range(2)]
    columns = planes * 2 * rows
    operands = [concentration, *tables[0], *tables[1], wave_x, twist_cos, twist_sin, *dft]
    f32, bf16 = jnp.float32, jnp.bfloat16
    back_rows = 2 * kk * planes
    dma = pltpu.SemaphoreType.DMA
    new_field, energy = pl.pallas_call(
        functools.partial(step_kernel, cells),
        out_shape=(
            jax.ShapeDtypeStruct(concentration.shape, f32),
            jax.ShapeDtypeStruct((1, 1), f32),
        ),
        in_specs=[pl.BlockSpec(memory_space=pltpu.VMEM)] * len(operands),
        out_specs=(
            pl.BlockSpec(memory_space=pltpu.VMEM),
            pl.BlockSpec(memory_space=pltpu.SMEM),
        ),
        scratch_shapes=[
            pltpu.VMEM((columns, half), bf16),
            pltpu.VMEM((columns, half), bf16),
            pltpu.VMEM((width, 2 * width), bf16),
            pltpu.VMEM((width, 2 * width), bf16),
            pltpu.VMEM((4, 2, 2 * full_z, kk + 8, width), f32),
            pltpu.VMEM((2, full_z, kk + 8, width), f32),
            pltpu.VMEM((4, 2, full_z, kk + 8, width), f32),
            pltpu.VMEM((planes * rows, half), f32),
            pltpu.VMEM((chunks, members, 2 * kk, columns), f32),
            pltpu.VMEM((chunks, members, 2 * kk, columns), f32),
            pltpu.VMEM((chunks, members, back_rows, rows), f32),
            pltpu.VMEM((chunks, members, back_rows, rows), f32),
            pltpu.VMEM((chunks, members, back_rows, rows), f32),
            pltpu.VMEM((chunks, members, back_rows, rows), f32),
            pltpu.VMEM((members, 8, lanes), f32),
            pltpu.VMEM((8, lanes), f32),
            pltpu.VMEM((8, lanes), f32),
            dma((chunks, members)),
            dma((chunks, members)),
            dma((chunks,)),
            dma((chunks,)),
            dma((chunks, members)),
            dma((chunks, members)),
            dma((members,)),
            dma((members,)),
            dma,
            dma,
        ],
        compiler_params=pltpu.CompilerParams(
            vmem_limit_bytes=vmem_limit, collective_id=0, has_side_effects=True
        ),
    )(*operands)
    return (new_field, energy.reshape(()))


def per_device(concentration):
    planes, rows, full_y = concentration.shape
    devices = lax.axis_size("slab") * lax.axis_size("section")
    share = full_y // 4 // devices
    fits = (
        rows == lanes
        and planes * lax.axis_size("section") == 4
        and 2 * share == row_group
        and devices == 32
        and lax.axis_size("section") == 2
    )
    return kernel_step(concentration) if fits else plain_step(concentration)


def solution(mesh):
    return jax.shard_map(
        per_device,
        mesh=mesh,
        in_specs=(P("section", "slab", None),),
        out_specs=(P("section", "slab", None), P()),
        check_vma=False,
    )
```

```python
import functools
import math

import jax
import jax.numpy as jnp
import numpy as np
from jax import lax
from jax.experimental import pallas as pl
from jax.experimental.pallas import tpu as pltpu
from jax.sharding import PartitionSpec as P

time_step = 100.0
kappa_grad = 2.0
stabilizer = 8.0
highest = lax.Precision.HIGHEST


def circle(length, first_total, second_total, direction):
    first_index = jnp.arange(first_total, dtype=jnp.int32)
    second_index = jnp.arange(second_total, dtype=jnp.int32)
    turn_index = first_index[:, None] * second_index[None, :] % length
    phase_angle = turn_index.astype(jnp.float32) * (2.0 * math.pi / length)
    return (jnp.cos(phase_angle), direction * jnp.sin(phase_angle))


def contract(pattern, real_part, imag_part, table_cos, table_sin):

    def product_of(operand, matrix):
        return jnp.einsum(pattern, operand, matrix, precision=highest)

    out_real = product_of(real_part, table_cos) - product_of(imag_part, table_sin)
    out_imag = product_of(real_part, table_sin) + product_of(imag_part, table_cos)
    return (out_real, out_imag)


def real_only(pattern, real_part, imag_part, table_cos, table_sin):
    return jnp.einsum(pattern, real_part, table_cos, precision=highest) - jnp.einsum(
        pattern, imag_part, table_sin, precision=highest
    )


def rotate(real_part, imag_part, table_cos, table_sin):
    return (
        real_part * table_cos - imag_part * table_sin,
        real_part * table_sin + imag_part * table_cos,
    )


def wave_square(storage, length, permuted):
    if permuted:
        actual = storage // 128 + length // 128 * (storage % 128)
    else:
        actual = storage
    signed = jnp.where(2 * actual >= length, actual - length, actual)
    phase_angle = signed.astype(jnp.float32) * (2.0 * math.pi / length)
    return phase_angle * phase_angle


def plain_step(concentration):
    plane_count, row_count, full_y = concentration.shape
    slab_count = lax.axis_size("slab")
    section_count = lax.axis_size("section")
    full_x = row_count * slab_count
    full_z = plane_count * section_count
    y_block = full_y // slab_count
    y_half = y_block // section_count
    blocks_x = full_x // 128
    blocks_y = full_y // 128
    cell_count = full_x * full_y * full_z
    slab_at = lax.axis_index("slab")
    section_at = lax.axis_index("section")
    squared = concentration * concentration
    bulk_sum = jnp.sum(0.25 * squared * squared - 0.5 * squared)
    cubic_term = squared * concentration - concentration
    shaped_c = concentration.reshape(1, plane_count, row_count, blocks_y, 128)
    shaped_g = cubic_term.reshape(1, plane_count, row_count, blocks_y, 128)
    first_cos, first_sin = circle(blocks_y, blocks_y, blocks_y, -1.0)
    part_real, part_imag = contract("fzxab,aj->fzxjb", shaped_c, shaped_g, first_cos, first_sin)
    field_total = part_real.shape[0]
    twist_cos, twist_sin = circle(full_y, blocks_y, 128, -1.0)
    part_real, part_imag = rotate(part_real, part_imag, twist_cos, twist_sin)
    lane_cos, lane_sin = circle(128, 128, 128, -1.0)
    part_real, part_imag = contract("fzxjb,bk->fxjkz", part_real, part_imag, lane_cos, lane_sin)
    outgoing = jnp.concatenate([part_real, part_imag], 0).reshape(
        2 * field_total, row_count, slab_count, y_block * plane_count
    )
    columns = lax.all_to_all(outgoing, "slab", split_axis=2, concat_axis=1, tiled=True)
    columns = columns.reshape(2 * field_total, blocks_x, 128, y_block * plane_count)
    first_cos, first_sin = circle(blocks_x, blocks_x, blocks_x, -1.0)
    part_real, part_imag = contract(
        "fabm,aj->fmjb", columns[:field_total], columns[field_total:], first_cos, first_sin
    )
    twist_cos, twist_sin = circle(full_x, blocks_x, 128, -1.0)
    part_real, part_imag = rotate(part_real, part_imag, twist_cos, twist_sin)
    part_real, part_imag = contract("fmjb,bk->fmjk", part_real, part_imag, lane_cos, lane_sin)
    spectra_x = jnp.concatenate([part_real, part_imag], 0).reshape(
        2 * field_total, y_block, plane_count, full_x
    )
    depth_cos, depth_sin = circle(full_z, full_z, full_z, -1.0)
    own_cos = lax.dynamic_slice_in_dim(depth_cos, section_at * plane_count, plane_count, 0)
    own_sin = lax.dynamic_slice_in_dim(depth_sin, section_at * plane_count, plane_count, 0)
    term_real, term_imag = contract(
        "fyzk,zq->yfqk", spectra_x[:field_total], spectra_x[field_total:], own_cos, own_sin
    )
    spectral = lax.psum_scatter(
        jnp.concatenate([term_real, term_imag], 1), "section", scatter_dimension=0, tiled=True
    )
    storage_y = slab_at * y_block + section_at * y_half + jnp.arange(y_half, dtype=jnp.int32)
    storage_x = jnp.arange(full_x, dtype=jnp.int32)
    storage_z = jnp.arange(full_z, dtype=jnp.int32)
    wave_sq = (
        wave_square(storage_y, full_y, True)[:, None, None]
        + wave_square(storage_z, full_z, False)[None, :, None]
        + wave_square(storage_x, full_x, True)[None, None, :]
    )
    numerator = 1.0 + time_step * stabilizer * wave_sq
    denominator = numerator + time_step * kappa_grad * wave_sq * wave_sq
    keep_rate = numerator / denominator
    mix_rate = time_step * wave_sq / denominator
    new_real = keep_rate * spectral[:, 0] - mix_rate * spectral[:, 1]
    new_imag = keep_rate * spectral[:, 1] + mix_rate * spectral[:, 0]
    back_cos, back_sin = circle(full_z, full_z, full_z, 1.0)
    part_real, part_imag = contract("yqk,qz->yzk", new_real, new_imag, back_cos, back_sin)
    returning = jnp.stack([part_real, part_imag], 1)
    own_planes = lax.all_to_all(returning, "section", split_axis=2, concat_axis=0, tiled=True)
    grid_real = own_planes[:, 0].reshape(y_block, plane_count, blocks_x, 128)
    grid_imag = own_planes[:, 1].reshape(y_block, plane_count, blocks_x, 128)
    lane_cos, lane_sin = circle(128, 128, 128, 1.0)
    part_real, part_imag = contract("szjk,kb->szjb", grid_real, grid_imag, lane_cos, lane_sin)
    twist_cos, twist_sin = circle(full_x, blocks_x, 128, 1.0)
    part_real, part_imag = rotate(part_real, part_imag, twist_cos, twist_sin)
    first_cos, first_sin = circle(blocks_x, blocks_x, blocks_x, 1.0)
    part_real, part_imag = contract("szjb,ja->absz", part_real, part_imag, first_cos, first_sin)
    leaving = jnp.stack([part_real, part_imag], 0).reshape(2, full_x, 1, y_block * plane_count)
    rows_back = lax.all_to_all(leaving, "slab", split_axis=1, concat_axis=2, tiled=True)
    rows_back = rows_back.reshape(2, row_count, blocks_y, 128, plane_count)
    part_real, part_imag = contract("xjkz,kb->xjbz", rows_back[0], rows_back[1], lane_cos, lane_sin)
    twist_cos, twist_sin = circle(full_y, blocks_y, 128, 1.0)
    part_real, part_imag = rotate(
        part_real, part_imag, twist_cos[:, :, None], twist_sin[:, :, None]
    )
    first_cos, first_sin = circle(blocks_y, blocks_y, blocks_y, 1.0)
    new_field = real_only("xjbz,ja->zxab", part_real, part_imag, first_cos, first_sin)
    new_field = new_field.reshape(plane_count, row_count, full_y) / cell_count
    total_bulk = lax.psum(bulk_sum, ("section", "slab"))
    energy = total_bulk / cell_count
    return (new_field, energy)


lanes = 128
row_group = 32
groups = 8
kk = 8
vmem_limit = 48 * 1024 * 1024
small_limit = 8 * 1024 * 1024


def split(values):
    high = values.astype(jnp.bfloat16)
    low = (values - high.astype(jnp.float32)).astype(jnp.bfloat16)
    return high, low


def triple(left_parts, right_parts, dims):
    def product(left, right):
        return lax.dot_general(left, right, (dims, ((), ())), preferred_element_type=jnp.float32)

    left_high, left_low = left_parts
    right_high, right_low = right_parts
    return (
        product(left_high, right_high)
        + product(left_low, right_high)
        + product(left_high, right_low)
    )


def y_tables(full_y, devices, parity):
    half = full_y // 2
    per_part = half // 2 // devices
    slot = np.arange(half)
    device, inner = slot // (2 * per_part), slot % (2 * per_part)
    part, local = inner // per_part, inner % per_part
    wave = parity + 2 * (device * per_part + local)
    position = np.arange(half)
    turns = wave[:, None] * position[None, :] % full_y
    phase = turns * (2.0 * math.pi / full_y)
    coarse = phase[::row_group]
    offset = wave[:row_group] - wave[0]
    fine = (offset[:, None] * position[None, :] % full_y) * (2.0 * math.pi / full_y)
    fine = fine + part[:row_group, None] * (0.5 * math.pi)
    return [
        table.astype(np.float32)
        for table in (np.cos(coarse), np.sin(coarse), np.cos(fine), np.sin(fine))
    ]


def y_block(refs, block, parity, kk):
    coarse_cos, coarse_sin, fine_cos, fine_sin = refs
    cos_fine, sin_fine = fine_cos[...], fine_sin[...]
    pieces = []
    for inner in range(groups):
        at = pl.ds(block * groups + inner, 1)
        piece = coarse_cos[at, :] * cos_fine - coarse_sin[at, :] * sin_fine
        if parity == 0 and inner == 0:
            row = lax.broadcasted_iota(jnp.int32, piece.shape, 0)
            column = lax.broadcasted_iota(jnp.int32, piece.shape, 1)
            sign = 1.0 - 2.0 * (column % 2).astype(jnp.float32)
            wanted = jnp.where(block == 0, kk, -1)
            piece = jnp.where(row == wanted, sign, piece)
        pieces.append(piece)
    return jnp.concatenate(pieces, 0)


def times_unit(real, imag, quarter_turns):
    turns = quarter_turns % 4
    if turns == 0:
        return real, imag
    if turns == 1:
        return -imag, real
    if turns == 2:
        return -real, -imag
    return imag, -real


def unit_sum(parts, power, direction):
    total_real, total_imag = parts[0]
    for index in range(1, len(parts)):
        real, imag = times_unit(*parts[index], direction * power * index)
        total_real = total_real + real
        total_imag = total_imag + imag
    return total_real, total_imag


def flip(bit, wanted):
    return 1 - bit if wanted else bit


class Place:
    def __init__(self):
        self.section = lax.axis_index("section")
        self.slab = lax.axis_index("slab")
        self.upper = self.slab // 8
        self.bits = [self.slab % 2, self.slab // 2 % 2, self.slab // 4 % 2, self.section]
        self.member = self.index_of(self.bits)

    @staticmethod
    def index_of(bits):
        return bits[3] * 8 + bits[2] * 4 + bits[1] * 2 + bits[0]

    def peer(self, turn):
        bits = [flip(bit, turn >> at & 1) for at, bit in enumerate(self.bits)]
        slab = self.upper * 8 + bits[2] * 4 + bits[1] * 2 + bits[0]
        return self.index_of(bits), (bits[3], slab)

    def partner(self):
        return self.section, (1 - self.upper) * 8 + self.slab % 8


def remote(source, target, send, receive, device):
    return pltpu.make_async_remote_copy(
        src_ref=source,
        dst_ref=target,
        send_sem=send,
        recv_sem=receive,
        device_id=device,
        device_id_type=pl.DeviceIdType.MESH,
    )


turn_order = list(range(1, 16))


def greet(place):
    barrier = pltpu.get_barrier_semaphore()
    devices = [place.peer(turn)[1] for turn in turn_order] + [place.partner()]
    for device in devices:
        pl.semaphore_signal(
            barrier, inc=1, device_id=device, device_id_type=pl.DeviceIdType.MESH
        )
    return lambda: pl.semaphore_wait(barrier, len(devices))


def step_kernel(cells, chunks, conc_from, y_from, x_from, *refs):
    even_ref, odd_ref, energy_ref = refs[0:3]
    (
        conc_ref, y_ref, x_ref, loaded,
        high_ref, low_ref, wide_high, wide_low, spec_ref, fil_ref,
        sent_ref, arrived_ref, own_ref, other_ref, partner_ref, returned_ref,
        tile_ref, half_ref, far_ref,
        sent_out, sent_in, other_out, other_in, own_out, own_in, tile_out, tile_in,
        half_out, half_in,
    ) = refs[3:]
    loads = [
        pltpu.make_async_copy(conc_from, conc_ref, loaded.at[0]),
        pltpu.make_async_copy(y_from.at[1], y_ref.at[1], loaded.at[1]),
        pltpu.make_async_copy(x_from, x_ref, loaded.at[2]),
        pltpu.make_async_copy(y_from.at[0], y_ref.at[0], loaded.at[3]),
    ]
    for load in loads:
        load.start()
    tables = [[y_ref.at[parity, at] for at in range(4)] for parity in range(2)]
    x_rows = x_ref.shape[0]
    short = row_group // 2
    starts = [0, 8, 16, 24, 24 + short, 24 + 2 * short, 24 + 2 * short + row_group]
    ends = starts[1:] + [x_rows]
    wx_ref, tw_cos, tw_sin, ca, sa, cb, sb = [
        x_ref.at[slice(start, end)] for start, end in zip(starts, ends)
    ]
    place = Place()
    member = place.member
    planes, rows, full_y = conc_ref.shape
    half = full_y // 2
    members, inner, columns = arrived_ref.shape[1:]
    width = spec_ref.shape[4]
    sections = 2
    full_z = planes * sections
    zf_local = planes * 2
    total_zf = zf_local * sections
    slabs = members // sections
    quarter = slabs // 2
    met = greet(place)

    def prepare(parity, wants_bulk):
        total = jnp.zeros((8, lanes), jnp.float32)
        for plane in range(planes):
            first = conc_ref[plane, :, :half]
            second = conc_ref[plane, :, half:]
            first_sq, second_sq = first * first, second * second
            if wants_bulk:
                bulk = 0.25 * (first_sq * first_sq + second_sq * second_sq)
                bulk = bulk - 0.5 * (first_sq + second_sq)
                bulk = jnp.sum(bulk.reshape(rows // 8, 8, half), axis=0)
                for at in range(0, half, lanes):
                    total = total + bulk[:, at : at + lanes]
            first_g = first_sq * first - first
            second_g = second_sq * second - second
            for field, (left, right) in enumerate(((first, second), (first_g, second_g))):
                mixed = left + right if parity == 0 else left - right
                high, low = split(mixed)
                at = (plane * 2 + field) * rows
                high_ref[at : at + rows, :] = high
                low_ref[at : at + rows, :] = low
        return total

    def forward(parity, sub, at):
        table = y_block(tables[parity], sub, parity, kk)
        result = triple(split(table), (high_ref[...], low_ref[...]), ((1,), (1,)))
        sent_ref[at] = result.reshape(members, inner, columns)
        arrived_ref[at, member] = sent_ref[at, member]

    def spread(at):
        copies = []
        for turn in turn_order:
            peer, device = place.peer(turn)
            copies.append(
                remote(
                    sent_ref.at[at, peer],
                    arrived_ref.at[at, member],
                    sent_out.at[at, turn],
                    sent_in.at[at, turn],
                    device,
                )
            )
        return copies

    def spread_tile():
        copies = []
        for turn in turn_order:
            copies.append(
                remote(
                    tile_ref.at[member],
                    tile_ref.at[member],
                    tile_out.at[turn],
                    tile_in.at[turn],
                    place.peer(turn)[1],
                )
            )
        return copies

    def wide_table():
        cos_rows, sin_rows = [], []
        cos_fine, sin_fine = cb[...], sb[...]
        for group in range(row_group // 2):
            cos_base, sin_base = ca[group : group + 1, :], sa[group : group + 1, :]
            cos_rows.append(cos_base * cos_fine - sin_base * sin_fine)
            sin_rows.append(sin_base * cos_fine + cos_base * sin_fine)
        table = jnp.concatenate([jnp.concatenate(cos_rows, 0), jnp.concatenate(sin_rows, 0)], 1)
        wide_high[...], wide_low[...] = split(table)

    def middle(chunk, has_extra):
        depth = 2 * kk if has_extra else kk
        sub = lax.rem(chunk, len(chunks) // 2)
        parity = jnp.where(chunk < len(chunks) // 2, 1, 0)
        base_wave = parity + 2 * kk * (sub * members + member)
        row_iota = lax.broadcasted_iota(jnp.int32, (kk, 1), 0)
        special = None
        if has_extra:
            wanted = jnp.where(member == 0, 0, -1)
            special = jnp.where(row_iota == wanted, 1.0, 0.0)

        def gather(section, a, part, zf):
            pieces = [
                arrived_ref[
                    chunk,
                    section * slabs + a * quarter + step,
                    part * kk : (part + 1) * kk,
                    zf * lanes : (zf + 1) * lanes,
                ]
                for step in range(quarter)
            ]
            return jnp.concatenate(pieces, 1)

        def put(parts, at, row):
            for j in range(4):
                real, imag = unit_sum(parts, j, -1)
                if j:
                    cos, sin = tw_cos[j : j + 1, :], tw_sin[j : j + 1, :]
                    real, imag = real * cos + imag * sin, imag * cos - real * sin
                spec_ref[j, 0, at, row : row + kk, :] = real
                spec_ref[j, 1, at, row : row + kk, :] = imag

        for section in range(sections):
            for zf in range(zf_local):
                at = section * zf_local + zf
                parts, extra = [], []
                for a in range(2):
                    real, imag = gather(section, a, 0, zf), gather(section, a, 1, zf)
                    if has_extra:
                        extra.append((imag * special, jnp.zeros_like(imag)))
                        imag = imag * (1.0 - special)
                    parts.append((real, imag))
                put(parts, at, 0)
                if has_extra:
                    put(extra, at, kk)

        weights = (wide_high[...], wide_low[...])

        def one(pair, carry):
            source = spec_ref[pl.ds(2 * pair, 2), :, :, 0:depth, :]
            raw = triple(split(source.reshape(4 * total_zf * depth, width)), weights, ((1,), (0,)))
            raw = raw.reshape(2, 2, total_zf, depth, 2 * width)
            for inside in range(2):
                j = 2 * pair + inside
                for row in range(0, depth, kk):
                    fields = []
                    for field in range(2):
                        per_z = []
                        for z in range(full_z):
                            re_part = raw[inside, 0, z * 2 + field, row : row + kk]
                            im_part = raw[inside, 1, z * 2 + field, row : row + kk]
                            per_z.append(
                                (
                                    re_part[:, :width] + im_part[:, width:],
                                    im_part[:, :width] - re_part[:, width:],
                                )
                            )
                        fields.append(per_z)
                    wave = base_wave + 2 * row_iota
                    if row:
                        wave = jnp.full_like(wave, half)
                    first = (wave == 0) | (wave == half)
                    weight = jnp.where(first, 1.0 / cells, 2.0 / cells)
                    angle = wave.astype(jnp.float32) * (2.0 * math.pi / full_y)
                    plane_sq = angle * angle + wx_ref[pl.ds(j, 1), :]
                    updated = []
                    for q in range(full_z):
                        c_real, c_imag = unit_sum(fields[0], q, -1)
                        g_real, g_imag = unit_sum(fields[1], q, -1)
                        signed = q - full_z if 2 * q >= full_z else q
                        wave_sq = plane_sq + (2.0 * math.pi * signed / full_z) ** 2
                        numerator = 1.0 + time_step * stabilizer * wave_sq
                        denominator = numerator + time_step * kappa_grad * wave_sq * wave_sq
                        inverse = weight / denominator
                        keep = numerator * inverse
                        mix = time_step * wave_sq * inverse
                        updated.append(
                            (keep * c_real - mix * g_real, keep * c_imag - mix * g_imag)
                        )
                    for z in range(full_z):
                        real, imag = unit_sum(updated, z, 1)
                        fil_ref[j, 0, z, row : row + kk, :] = real
                        fil_ref[j, 1, z, row : row + kk, :] = imag
            return carry

        lax.fori_loop(0, 2, one, 0)
        source = fil_ref[:, :, :, 0:depth, :].reshape(8 * full_z * depth, width)
        raw = triple(split(source), weights, ((1,), (0,))).reshape(4, 2, full_z, depth, 2 * width)

        def back(z, row):
            parts = []
            for j in range(4):
                re_part = raw[j, 0, z, row : row + kk]
                im_part = raw[j, 1, z, row : row + kk]
                real = re_part[:, :width] - im_part[:, width:]
                imag = re_part[:, width:] + im_part[:, :width]
                if j:
                    cos, sin = tw_cos[j : j + 1, :], tw_sin[j : j + 1, :]
                    real, imag = real * cos - imag * sin, imag * cos + real * sin
                parts.append((real, imag))
            return parts

        for z in range(full_z):
            section, plane = z // planes, z % planes
            parts = back(z, 0)
            extra = back(z, kk) if has_extra else None
            for a in range(4):
                real, imag = unit_sum(parts, a, 1)
                if has_extra:
                    extra_real, _ = unit_sum(extra, a, 1)
                    imag = imag * (1.0 - special) + extra_real * special
                target_ref = own_ref if a < 2 else other_ref
                for step in range(quarter):
                    target = section * slabs + a % 2 * quarter + step
                    piece = slice(step * lanes, (step + 1) * lanes)
                    at = plane * inner
                    target_ref[chunk, target, at : at + kk, :] = real[:, piece]
                    target_ref[chunk, target, at + kk : at + 2 * kk, :] = imag[:, piece]

    def cross(chunk):
        return remote(
            other_ref.at[chunk],
            partner_ref.at[chunk],
            other_out.at[chunk],
            other_in.at[chunk],
            place.partner(),
        )

    def far():
        return remote(half_ref, far_ref, half_out, half_in, place.partner())

    def join(chunk):
        wait_in([cross(chunk)])
        own_ref[chunk] = own_ref[chunk] + partner_ref[chunk]
        returned_ref[chunk, member] = own_ref[chunk, member]
        start(give_back(chunk))

    def give_back(chunk):
        copies = []
        for turn in turn_order:
            peer, device = place.peer(turn)
            copies.append(
                remote(
                    own_ref.at[chunk, peer],
                    returned_ref.at[chunk, member],
                    own_out.at[chunk, turn],
                    own_in.at[chunk, turn],
                    device,
                )
            )
        return copies

    def backward(parity, sub, chunk):
        turned = [
            returned_ref[chunk, :, plane * inner : (plane + 1) * inner, :]
            .reshape(members * inner, rows)
            .T
            for plane in range(planes)
        ]
        table = y_block(tables[parity], sub, parity, kk)
        term = triple(split(jnp.concatenate(turned, 0)), split(table), ((1,), (0,)))
        target = (even_ref, odd_ref)[parity]
        target[...] = target[...] + term

    def start(copies):
        for copy in copies:
            copy.start()

    def wait_in(copies):
        for copy in copies:
            copy.wait_recv()

    total = len(chunks)
    special_at = chunks.index((0, 0))
    subs = total // 2
    lead = 2
    even_ref[...] = jnp.zeros_like(even_ref)
    odd_ref[...] = jnp.zeros_like(odd_ref)
    loads[0].wait()
    tile_ref[member] = prepare(1, True)
    loads[1].wait()
    forward(1, 0, 0)
    met()
    start(spread(0))
    start(spread_tile())
    forward(1, 1, 1)
    start(spread(1))
    loads[2].wait()
    wide_table()
    lax.fori_loop(2, subs, lambda at, carry: forward(1, at, at), None)
    prepare(0, False)
    loads[3].wait()
    lax.fori_loop(0, subs, lambda at, carry: forward(0, at, subs + at), None)

    def one(at, carry):
        wait_in(spread(at))

        @pl.when(at != special_at)
        def _():
            middle(at, False)

        @pl.when(at == special_at)
        def _():
            middle(at, True)

        start([cross(at)])

        @pl.when(at + lead < total)
        def _():
            start(spread(at + lead))

        @pl.when(at == 0)
        def _():
            wait_in(spread_tile())
            half_ref[...] = jnp.sum(tile_ref[...], axis=0)
            start([far()])

        @pl.when(at >= 2)
        def _():
            join(at - 2)

        @pl.when(at >= subs)
        def _():
            wait_in(give_back(at - subs))
            backward(1, at - subs, at - subs)

        return carry

    lax.fori_loop(0, total, one, 0)
    wait_in([far()])
    energy_ref[0, 0] = jnp.sum(half_ref[...] + far_ref[...]) / cells

    def last(at, carry):
        @pl.when(at < 2)
        def _():
            join(at + total - 2)

        wait_in(give_back(at + subs))
        backward(0, at, at + subs)
        return carry

    lax.fori_loop(0, subs, last, 0)

    def sent(at, carry):
        for copy in spread(at) + give_back(at) + [cross(at)]:
            copy.wait_send()
        return carry

    lax.fori_loop(0, total, sent, 0)
    for copy in spread_tile() + [far()]:
        copy.wait_send()


def combine_kernel(even_ref, odd_ref, out_ref):
    planes, rows, full_y = out_ref.shape
    half = full_y // 2
    for plane in range(planes):
        even_rows = even_ref[plane * rows : (plane + 1) * rows, :]
        odd_rows = odd_ref[plane * rows : (plane + 1) * rows, :]
        out_ref[plane, :, :half] = even_rows + odd_rows
        out_ref[plane, :, half:] = even_rows - odd_rows


def kernel_step(concentration):
    planes, rows, full_y = concentration.shape
    slabs = lax.axis_size("slab")
    sections = lax.axis_size("section")
    members = slabs * sections // 2
    full_x = rows * slabs
    full_z = planes * sections
    cells = full_x * full_y * full_z
    half = full_y // 2
    subs = half // 2 // members // kk
    width = full_x // 4
    base = np.arange(width)
    step = 2.0 * math.pi / width
    coarse = base[::row_group, None] * base[None, :] % width * step
    fine = base[:row_group, None] * base[None, :] % width * step
    dft = [f(t).astype(np.float32) for t in (coarse, fine) for f in (np.cos, np.sin)]
    twist = np.arange(4)[:, None] * base[None, :] * (2.0 * math.pi / full_x)
    twist_cos, twist_sin = np.cos(twist).astype(np.float32), np.sin(twist).astype(np.float32)
    kx = np.arange(4)[:, None] + 4 * base[None, :]
    kx = np.where(2 * kx >= full_x, kx - full_x, kx) * (2.0 * math.pi / full_x)
    wave_x = (kx * kx).astype(np.float32)
    tables = [y_tables(full_y, members * subs, parity) for parity in range(2)]
    chunks = [(1, sub) for sub in range(subs)] + [(0, sub) for sub in range(subs)]
    count = len(chunks)
    columns = planes * 2 * rows
    y_rows = np.stack([np.stack(parts) for parts in tables])
    small = [np.concatenate([rows, rows]) for rows in (wave_x, twist_cos, twist_sin)]
    coarse_cos, coarse_sin, fine_cos, fine_sin = dft
    x_rows = np.concatenate([*small, coarse_cos, coarse_sin, fine_cos, fine_sin])
    operands = [concentration, y_rows, x_rows]
    f32, bf16 = jnp.float32, jnp.bfloat16
    vmem, dma = pltpu.VMEM, pltpu.SemaphoreType.DMA
    in_vmem = pl.BlockSpec(memory_space=pltpu.VMEM)
    forth = vmem((count, members, 2 * kk, columns), f32)
    half_back = vmem((count, members, 2 * kk * planes, rows), f32)
    even, odd, energy = pl.pallas_call(
        functools.partial(step_kernel, cells, chunks),
        out_shape=(
            jax.ShapeDtypeStruct((planes * rows, half), f32),
            jax.ShapeDtypeStruct((planes * rows, half), f32),
            jax.ShapeDtypeStruct((1, 1), f32),
        ),
        in_specs=[pl.BlockSpec(memory_space=pltpu.HBM)] * len(operands),
        out_specs=(in_vmem, in_vmem, pl.BlockSpec(memory_space=pltpu.SMEM)),
        scratch_shapes=[
            vmem(concentration.shape, f32),
            vmem(y_rows.shape, f32),
            vmem(x_rows.shape, f32),
            dma((4,)),
            vmem((columns, half), bf16),
            vmem((columns, half), bf16),
            vmem((width, 2 * width), bf16),
            vmem((width, 2 * width), bf16),
            vmem((4, 2, 2 * full_z, 2 * kk, width), f32),
            vmem((4, 2, full_z, 2 * kk, width), f32),
            forth,
            forth,
            half_back,
            half_back,
            half_back,
            half_back,
            vmem((members, 8, lanes), f32),
            vmem((8, lanes), f32),
            vmem((8, lanes), f32),
            dma((count, members)),
            dma((count, members)),
            dma((count,)),
            dma((count,)),
            dma((count, members)),
            dma((count, members)),
            dma((members,)),
            dma((members,)),
            dma,
            dma,
        ],
        compiler_params=pltpu.CompilerParams(
            vmem_limit_bytes=vmem_limit, collective_id=0, has_side_effects=True
        ),
    )(*[pltpu.with_memory_space_constraint(jnp.asarray(x), pltpu.HBM) for x in operands])
    new_field = pl.pallas_call(
        combine_kernel,
        out_shape=jax.ShapeDtypeStruct(concentration.shape, f32),
        in_specs=[in_vmem] * 2,
        out_specs=in_vmem,
        compiler_params=pltpu.CompilerParams(vmem_limit_bytes=small_limit),
    )(even, odd)
    return (new_field, energy.reshape(()))


def per_device(concentration):
    planes, rows, full_y = concentration.shape
    devices = lax.axis_size("slab") * lax.axis_size("section")
    share = full_y // 4 // devices
    fits = (
        rows == lanes
        and planes * lax.axis_size("section") == 4
        and share == 2 * kk
        and devices == 32
        and lax.axis_size("section") == 2
    )
    return kernel_step(concentration) if fits else plain_step(concentration)


def solution(mesh):
    return jax.shard_map(
        per_device,
        mesh=mesh,
        in_specs=(P("section", "slab", None),),
        out_specs=(P("section", "slab", None), P()),
        check_vma=False,
    )
```

```python
import functools
import math

import jax
import jax.numpy as jnp
import numpy as np
from jax import lax
from jax.experimental import pallas as pl
from jax.experimental.pallas import tpu as pltpu
from jax.sharding import PartitionSpec as P

time_step = 100.0
kappa_grad = 2.0
stabilizer = 8.0
highest = lax.Precision.HIGHEST


def circle(length, first_total, second_total, direction):
    first_index = jnp.arange(first_total, dtype=jnp.int32)
    second_index = jnp.arange(second_total, dtype=jnp.int32)
    turn_index = first_index[:, None] * second_index[None, :] % length
    phase_angle = turn_index.astype(jnp.float32) * (2.0 * math.pi / length)
    return (jnp.cos(phase_angle), direction * jnp.sin(phase_angle))


def contract(pattern, real_part, imag_part, table_cos, table_sin):

    def product_of(operand, matrix):
        return jnp.einsum(pattern, operand, matrix, precision=highest)

    out_real = product_of(real_part, table_cos) - product_of(imag_part, table_sin)
    out_imag = product_of(real_part, table_sin) + product_of(imag_part, table_cos)
    return (out_real, out_imag)


def real_only(pattern, real_part, imag_part, table_cos, table_sin):
    return jnp.einsum(pattern, real_part, table_cos, precision=highest) - jnp.einsum(
        pattern, imag_part, table_sin, precision=highest
    )


def rotate(real_part, imag_part, table_cos, table_sin):
    return (
        real_part * table_cos - imag_part * table_sin,
        real_part * table_sin + imag_part * table_cos,
    )


def wave_square(storage, length, permuted):
    if permuted:
        actual = storage // 128 + length // 128 * (storage % 128)
    else:
        actual = storage
    signed = jnp.where(2 * actual >= length, actual - length, actual)
    phase_angle = signed.astype(jnp.float32) * (2.0 * math.pi / length)
    return phase_angle * phase_angle


def plain_step(concentration):
    plane_count, row_count, full_y = concentration.shape
    slab_count = lax.axis_size("slab")
    section_count = lax.axis_size("section")
    full_x = row_count * slab_count
    full_z = plane_count * section_count
    y_block = full_y // slab_count
    y_half = y_block // section_count
    blocks_x = full_x // 128
    blocks_y = full_y // 128
    cell_count = full_x * full_y * full_z
    slab_at = lax.axis_index("slab")
    section_at = lax.axis_index("section")
    squared = concentration * concentration
    bulk_sum = jnp.sum(0.25 * squared * squared - 0.5 * squared)
    cubic_term = squared * concentration - concentration
    shaped_c = concentration.reshape(1, plane_count, row_count, blocks_y, 128)
    shaped_g = cubic_term.reshape(1, plane_count, row_count, blocks_y, 128)
    first_cos, first_sin = circle(blocks_y, blocks_y, blocks_y, -1.0)
    part_real, part_imag = contract("fzxab,aj->fzxjb", shaped_c, shaped_g, first_cos, first_sin)
    field_total = part_real.shape[0]
    twist_cos, twist_sin = circle(full_y, blocks_y, 128, -1.0)
    part_real, part_imag = rotate(part_real, part_imag, twist_cos, twist_sin)
    lane_cos, lane_sin = circle(128, 128, 128, -1.0)
    part_real, part_imag = contract("fzxjb,bk->fxjkz", part_real, part_imag, lane_cos, lane_sin)
    outgoing = jnp.concatenate([part_real, part_imag], 0).reshape(
        2 * field_total, row_count, slab_count, y_block * plane_count
    )
    columns = lax.all_to_all(outgoing, "slab", split_axis=2, concat_axis=1, tiled=True)
    columns = columns.reshape(2 * field_total, blocks_x, 128, y_block * plane_count)
    first_cos, first_sin = circle(blocks_x, blocks_x, blocks_x, -1.0)
    part_real, part_imag = contract(
        "fabm,aj->fmjb", columns[:field_total], columns[field_total:], first_cos, first_sin
    )
    twist_cos, twist_sin = circle(full_x, blocks_x, 128, -1.0)
    part_real, part_imag = rotate(part_real, part_imag, twist_cos, twist_sin)
    part_real, part_imag = contract("fmjb,bk->fmjk", part_real, part_imag, lane_cos, lane_sin)
    spectra_x = jnp.concatenate([part_real, part_imag], 0).reshape(
        2 * field_total, y_block, plane_count, full_x
    )
    depth_cos, depth_sin = circle(full_z, full_z, full_z, -1.0)
    own_cos = lax.dynamic_slice_in_dim(depth_cos, section_at * plane_count, plane_count, 0)
    own_sin = lax.dynamic_slice_in_dim(depth_sin, section_at * plane_count, plane_count, 0)
    term_real, term_imag = contract(
        "fyzk,zq->yfqk", spectra_x[:field_total], spectra_x[field_total:], own_cos, own_sin
    )
    spectral = lax.psum_scatter(
        jnp.concatenate([term_real, term_imag], 1), "section", scatter_dimension=0, tiled=True
    )
    storage_y = slab_at * y_block + section_at * y_half + jnp.arange(y_half, dtype=jnp.int32)
    storage_x = jnp.arange(full_x, dtype=jnp.int32)
    storage_z = jnp.arange(full_z, dtype=jnp.int32)
    wave_sq = (
        wave_square(storage_y, full_y, True)[:, None, None]
        + wave_square(storage_z, full_z, False)[None, :, None]
        + wave_square(storage_x, full_x, True)[None, None, :]
    )
    numerator = 1.0 + time_step * stabilizer * wave_sq
    denominator = numerator + time_step * kappa_grad * wave_sq * wave_sq
    keep_rate = numerator / denominator
    mix_rate = time_step * wave_sq / denominator
    new_real = keep_rate * spectral[:, 0] - mix_rate * spectral[:, 1]
    new_imag = keep_rate * spectral[:, 1] + mix_rate * spectral[:, 0]
    back_cos, back_sin = circle(full_z, full_z, full_z, 1.0)
    part_real, part_imag = contract("yqk,qz->yzk", new_real, new_imag, back_cos, back_sin)
    returning = jnp.stack([part_real, part_imag], 1)
    own_planes = lax.all_to_all(returning, "section", split_axis=2, concat_axis=0, tiled=True)
    grid_real = own_planes[:, 0].reshape(y_block, plane_count, blocks_x, 128)
    grid_imag = own_planes[:, 1].reshape(y_block, plane_count, blocks_x, 128)
    lane_cos, lane_sin = circle(128, 128, 128, 1.0)
    part_real, part_imag = contract("szjk,kb->szjb", grid_real, grid_imag, lane_cos, lane_sin)
    twist_cos, twist_sin = circle(full_x, blocks_x, 128, 1.0)
    part_real, part_imag = rotate(part_real, part_imag, twist_cos, twist_sin)
    first_cos, first_sin = circle(blocks_x, blocks_x, blocks_x, 1.0)
    part_real, part_imag = contract("szjb,ja->absz", part_real, part_imag, first_cos, first_sin)
    leaving = jnp.stack([part_real, part_imag], 0).reshape(2, full_x, 1, y_block * plane_count)
    rows_back = lax.all_to_all(leaving, "slab", split_axis=1, concat_axis=2, tiled=True)
    rows_back = rows_back.reshape(2, row_count, blocks_y, 128, plane_count)
    part_real, part_imag = contract("xjkz,kb->xjbz", rows_back[0], rows_back[1], lane_cos, lane_sin)
    twist_cos, twist_sin = circle(full_y, blocks_y, 128, 1.0)
    part_real, part_imag = rotate(
        part_real, part_imag, twist_cos[:, :, None], twist_sin[:, :, None]
    )
    first_cos, first_sin = circle(blocks_y, blocks_y, blocks_y, 1.0)
    new_field = real_only("xjbz,ja->zxab", part_real, part_imag, first_cos, first_sin)
    new_field = new_field.reshape(plane_count, row_count, full_y) / cell_count
    total_bulk = lax.psum(bulk_sum, ("section", "slab"))
    energy = total_bulk / cell_count
    return (new_field, energy)


lanes = 128
row_group = 32
groups = 8
kk = 8
vmem_limit = 48 * 1024 * 1024
small_limit = 8 * 1024 * 1024


def split(values):
    high = values.astype(jnp.bfloat16)
    low = (values - high.astype(jnp.float32)).astype(jnp.bfloat16)
    return high, low


def triple(left_parts, right_parts, dims):
    def product(left, right):
        return lax.dot_general(left, right, (dims, ((), ())), preferred_element_type=jnp.float32)

    left_high, left_low = left_parts
    right_high, right_low = right_parts
    return (
        product(left_high, right_high)
        + product(left_low, right_high)
        + product(left_high, right_low)
    )


def y_tables(full_y, devices, parity):
    half = full_y // 2
    per_part = half // 2 // devices
    slot = np.arange(half)
    device, inner = slot // (2 * per_part), slot % (2 * per_part)
    part, local = inner // per_part, inner % per_part
    wave = parity + 2 * (device * per_part + local)
    position = np.arange(half)
    turns = wave[:, None] * position[None, :] % full_y
    phase = turns * (2.0 * math.pi / full_y)
    coarse = phase[::row_group]
    offset = wave[:row_group] - wave[0]
    fine = (offset[:, None] * position[None, :] % full_y) * (2.0 * math.pi / full_y)
    fine = fine + part[:row_group, None] * (0.5 * math.pi)
    return [
        table.astype(np.float32)
        for table in (np.cos(coarse), np.sin(coarse), np.cos(fine), np.sin(fine))
    ]


def y_block(refs, block, parity, kk):
    coarse_cos, coarse_sin, fine_cos, fine_sin = refs
    cos_fine, sin_fine = fine_cos[...], fine_sin[...]
    pieces = []
    for inner in range(groups):
        at = pl.ds(block * groups + inner, 1)
        piece = coarse_cos[at, :] * cos_fine - coarse_sin[at, :] * sin_fine
        if parity == 0 and inner == 0:
            row = lax.broadcasted_iota(jnp.int32, piece.shape, 0)
            column = lax.broadcasted_iota(jnp.int32, piece.shape, 1)
            sign = 1.0 - 2.0 * (column % 2).astype(jnp.float32)
            wanted = jnp.where(block == 0, kk, -1)
            piece = jnp.where(row == wanted, sign, piece)
        pieces.append(piece)
    return jnp.concatenate(pieces, 0)


def times_unit(real, imag, quarter_turns):
    turns = quarter_turns % 4
    if turns == 0:
        return real, imag
    if turns == 1:
        return -imag, real
    if turns == 2:
        return -real, -imag
    return imag, -real


def unit_sum(parts, power, direction):
    total_real, total_imag = parts[0]
    for index in range(1, len(parts)):
        real, imag = times_unit(*parts[index], direction * power * index)
        total_real = total_real + real
        total_imag = total_imag + imag
    return total_real, total_imag


def flip(bit, wanted):
    return 1 - bit if wanted else bit


class Place:
    def __init__(self):
        self.section = lax.axis_index("section")
        self.slab = lax.axis_index("slab")
        self.upper = self.slab // 8
        self.bits = [self.slab % 2, self.slab // 2 % 2, self.slab // 4 % 2, self.section]
        self.member = self.index_of(self.bits)

    @staticmethod
    def index_of(bits):
        return bits[3] * 8 + bits[2] * 4 + bits[1] * 2 + bits[0]

    def peer(self, turn):
        bits = [flip(bit, turn >> at & 1) for at, bit in enumerate(self.bits)]
        slab = self.upper * 8 + bits[2] * 4 + bits[1] * 2 + bits[0]
        return self.index_of(bits), (bits[3], slab)

    def partner(self):
        return self.section, (1 - self.upper) * 8 + self.slab % 8


def remote(source, target, send, receive, device):
    return pltpu.make_async_remote_copy(
        src_ref=source,
        dst_ref=target,
        send_sem=send,
        recv_sem=receive,
        device_id=device,
        device_id_type=pl.DeviceIdType.MESH,
    )


turn_order = list(range(1, 16))


def greet(place):
    barrier = pltpu.get_barrier_semaphore()
    devices = [place.peer(turn)[1] for turn in turn_order] + [place.partner()]
    for device in devices:
        pl.semaphore_signal(
            barrier, inc=1, device_id=device, device_id_type=pl.DeviceIdType.MESH
        )
    return lambda: pl.semaphore_wait(barrier, len(devices))


def step_kernel(cells, chunks, conc_from, y_from, x_from, *refs):
    even_ref, odd_ref, energy_ref = refs[0:3]
    (
        conc_ref, y_ref, x_ref, loaded,
        high_ref, low_ref, wide_high, wide_low, spec_ref, fil_ref,
        sent_ref, arrived_ref, own_ref, other_ref, partner_ref, returned_ref,
        tile_ref, half_ref, far_ref,
        sent_out, sent_in, other_out, other_in, own_out, own_in, tile_out, tile_in,
        half_out, half_in,
    ) = refs[3:]
    loads = [
        pltpu.make_async_copy(conc_from, conc_ref, loaded.at[0]),
        pltpu.make_async_copy(y_from.at[1], y_ref.at[1], loaded.at[1]),
        pltpu.make_async_copy(x_from, x_ref, loaded.at[2]),
        pltpu.make_async_copy(y_from.at[0], y_ref.at[0], loaded.at[3]),
    ]
    for load in loads:
        load.start()
    tables = [[y_ref.at[parity, at] for at in range(4)] for parity in range(2)]
    x_rows = x_ref.shape[0]
    short = row_group // 2
    starts = [0, 8, 16, 24, 24 + short, 24 + 2 * short, 24 + 2 * short + row_group]
    ends = starts[1:] + [x_rows]
    wx_ref, tw_cos, tw_sin, ca, sa, cb, sb = [
        x_ref.at[slice(start, end)] for start, end in zip(starts, ends)
    ]
    place = Place()
    member = place.member
    planes, rows, full_y = conc_ref.shape
    half = full_y // 2
    members, inner, columns = arrived_ref.shape[1:]
    width = spec_ref.shape[4]
    sections = 2
    full_z = planes * sections
    zf_local = planes * 2
    total_zf = zf_local * sections
    slabs = members // sections
    quarter = slabs // 2
    met = greet(place)

    def prepare(parity, wants_bulk):
        total = jnp.zeros((8, lanes), jnp.float32)
        for plane in range(planes):
            first = conc_ref[plane, :, :half]
            second = conc_ref[plane, :, half:]
            first_sq, second_sq = first * first, second * second
            if wants_bulk:
                bulk = 0.25 * (first_sq * first_sq + second_sq * second_sq)
                bulk = bulk - 0.5 * (first_sq + second_sq)
                bulk = jnp.sum(bulk.reshape(rows // 8, 8, half), axis=0)
                for at in range(0, half, lanes):
                    total = total + bulk[:, at : at + lanes]
            first_g = first_sq * first - first
            second_g = second_sq * second - second
            for field, (left, right) in enumerate(((first, second), (first_g, second_g))):
                mixed = left + right if parity == 0 else left - right
                high, low = split(mixed)
                at = (plane * 2 + field) * rows
                high_ref[at : at + rows, :] = high
                low_ref[at : at + rows, :] = low
        return total

    def forward(parity, sub, at):
        table = y_block(tables[parity], sub, parity, kk)
        result = triple(split(table), (high_ref[...], low_ref[...]), ((1,), (1,)))
        sent_ref[at] = result.reshape(members, inner, columns)
        arrived_ref[at, member] = sent_ref[at, member]

    def spread(at):
        copies = []
        for turn in turn_order:
            peer, device = place.peer(turn)
            copies.append(
                remote(
                    sent_ref.at[at, peer],
                    arrived_ref.at[at, member],
                    sent_out.at[at],
                    sent_in.at[at],
                    device,
                )
            )
        return copies

    def spread_tile():
        copies = []
        for turn in turn_order:
            copies.append(
                remote(
                    tile_ref.at[member],
                    tile_ref.at[member],
                    tile_out,
                    tile_in,
                    place.peer(turn)[1],
                )
            )
        return copies

    def wide_table():
        cos_rows, sin_rows = [], []
        cos_fine, sin_fine = cb[...], sb[...]
        for group in range(row_group // 2):
            cos_base, sin_base = ca[group : group + 1, :], sa[group : group + 1, :]
            cos_rows.append(cos_base * cos_fine - sin_base * sin_fine)
            sin_rows.append(sin_base * cos_fine + cos_base * sin_fine)
        table = jnp.concatenate([jnp.concatenate(cos_rows, 0), jnp.concatenate(sin_rows, 0)], 1)
        wide_high[...], wide_low[...] = split(table)

    def middle(chunk, has_extra):
        depth = 2 * kk if has_extra else kk
        sub = lax.rem(chunk, len(chunks) // 2)
        parity = jnp.where(chunk < len(chunks) // 2, 1, 0)
        base_wave = parity + 2 * kk * (sub * members + member)
        row_iota = lax.broadcasted_iota(jnp.int32, (kk, 1), 0)
        special = None
        if has_extra:
            wanted = jnp.where(member == 0, 0, -1)
            special = jnp.where(row_iota == wanted, 1.0, 0.0)

        def gather(section, a, part, zf):
            pieces = [
                arrived_ref[
                    chunk,
                    section * slabs + a * quarter + step,
                    part * kk : (part + 1) * kk,
                    zf * lanes : (zf + 1) * lanes,
                ]
                for step in range(quarter)
            ]
            return jnp.concatenate(pieces, 1)

        def put(parts, at, row):
            for j in range(4):
                real, imag = unit_sum(parts, j, -1)
                if j:
                    cos, sin = tw_cos[j : j + 1, :], tw_sin[j : j + 1, :]
                    real, imag = real * cos + imag * sin, imag * cos - real * sin
                spec_ref[j, 0, at, row : row + kk, :] = real
                spec_ref[j, 1, at, row : row + kk, :] = imag

        for section in range(sections):
            for zf in range(zf_local):
                at = section * zf_local + zf
                parts, extra = [], []
                for a in range(2):
                    real, imag = gather(section, a, 0, zf), gather(section, a, 1, zf)
                    if has_extra:
                        extra.append((imag * special, jnp.zeros_like(imag)))
                        imag = imag * (1.0 - special)
                    parts.append((real, imag))
                put(parts, at, 0)
                if has_extra:
                    put(extra, at, kk)

        weights = (wide_high[...], wide_low[...])

        def one(pair, carry):
            source = spec_ref[pl.ds(2 * pair, 2), :, :, 0:depth, :]
            raw = triple(split(source.reshape(4 * total_zf * depth, width)), weights, ((1,), (0,)))
            raw = raw.reshape(2, 2, total_zf, depth, 2 * width)
            for inside in range(2):
                j = 2 * pair + inside
                for row in range(0, depth, kk):
                    fields = []
                    for field in range(2):
                        per_z = []
                        for z in range(full_z):
                            re_part = raw[inside, 0, z * 2 + field, row : row + kk]
                            im_part = raw[inside, 1, z * 2 + field, row : row + kk]
                            per_z.append(
                                (
                                    re_part[:, :width] + im_part[:, width:],
                                    im_part[:, :width] - re_part[:, width:],
                                )
                            )
                        fields.append(per_z)
                    wave = base_wave + 2 * row_iota
                    if row:
                        wave = jnp.full_like(wave, half)
                    first = (wave == 0) | (wave == half)
                    weight = jnp.where(first, 1.0 / cells, 2.0 / cells)
                    angle = wave.astype(jnp.float32) * (2.0 * math.pi / full_y)
                    plane_sq = angle * angle + wx_ref[pl.ds(j, 1), :]
                    updated = []
                    for q in range(full_z):
                        c_real, c_imag = unit_sum(fields[0], q, -1)
                        g_real, g_imag = unit_sum(fields[1], q, -1)
                        signed = q - full_z if 2 * q >= full_z else q
                        wave_sq = plane_sq + (2.0 * math.pi * signed / full_z) ** 2
                        numerator = 1.0 + time_step * stabilizer * wave_sq
                        denominator = numerator + time_step * kappa_grad * wave_sq * wave_sq
                        inverse = weight / denominator
                        keep = numerator * inverse
                        mix = time_step * wave_sq * inverse
                        updated.append(
                            (keep * c_real - mix * g_real, keep * c_imag - mix * g_imag)
                        )
                    for z in range(full_z):
                        real, imag = unit_sum(updated, z, 1)
                        fil_ref[j, 0, z, row : row + kk, :] = real
                        fil_ref[j, 1, z, row : row + kk, :] = imag
            return carry

        lax.fori_loop(0, 2, one, 0)
        source = fil_ref[:, :, :, 0:depth, :].reshape(8 * full_z * depth, width)
        raw = triple(split(source), weights, ((1,), (0,))).reshape(4, 2, full_z, depth, 2 * width)

        def back(z, row):
            parts = []
            for j in range(4):
                re_part = raw[j, 0, z, row : row + kk]
                im_part = raw[j, 1, z, row : row + kk]
                real = re_part[:, :width] - im_part[:, width:]
                imag = re_part[:, width:] + im_part[:, :width]
                if j:
                    cos, sin = tw_cos[j : j + 1, :], tw_sin[j : j + 1, :]
                    real, imag = real * cos - imag * sin, imag * cos + real * sin
                parts.append((real, imag))
            return parts

        for z in range(full_z):
            section, plane = z // planes, z % planes
            parts = back(z, 0)
            extra = back(z, kk) if has_extra else None
            for a in range(4):
                real, imag = unit_sum(parts, a, 1)
                if has_extra:
                    extra_real, _ = unit_sum(extra, a, 1)
                    imag = imag * (1.0 - special) + extra_real * special
                target_ref = own_ref if a < 2 else other_ref
                for step in range(quarter):
                    target = section * slabs + a % 2 * quarter + step
                    piece = slice(step * lanes, (step + 1) * lanes)
                    at = plane * inner
                    target_ref[chunk, target, at : at + kk, :] = real[:, piece]
                    target_ref[chunk, target, at + kk : at + 2 * kk, :] = imag[:, piece]

    def cross(chunk):
        return remote(
            other_ref.at[chunk],
            partner_ref.at[chunk],
            other_out.at[chunk],
            other_in.at[chunk],
            place.partner(),
        )

    def far():
        return remote(half_ref, far_ref, half_out, half_in, place.partner())

    def join(chunk):
        cross(chunk).wait_recv()
        own_ref[chunk] = own_ref[chunk] + partner_ref[chunk]
        returned_ref[chunk, member] = own_ref[chunk, member]
        start(give_back(chunk))

    def give_back(chunk):
        copies = []
        for turn in turn_order:
            peer, device = place.peer(turn)
            copies.append(
                remote(
                    own_ref.at[chunk, peer],
                    returned_ref.at[chunk, member],
                    own_out.at[chunk],
                    own_in.at[chunk],
                    device,
                )
            )
        return copies

    def backward(parity, sub, chunk):
        turned = [
            returned_ref[chunk, :, plane * inner : (plane + 1) * inner, :]
            .reshape(members * inner, rows)
            .T
            for plane in range(planes)
        ]
        table = y_block(tables[parity], sub, parity, kk)
        term = triple(split(jnp.concatenate(turned, 0)), split(table), ((1,), (0,)))
        target = (even_ref, odd_ref)[parity]
        target[...] = target[...] + term

    def spread_all(at):
        return remote(
            sent_ref.at[at, 0 : members - 1],
            arrived_ref.at[at, 0 : members - 1],
            sent_out.at[at],
            sent_in.at[at],
            place.partner(),
        )

    def tile_all():
        part = tile_ref.at[0 : members - 1]
        return remote(part, part, tile_out, tile_in, place.partner())

    def back_all(at):
        return remote(
            own_ref.at[at, 0 : members - 1],
            returned_ref.at[at, 0 : members - 1],
            own_out.at[at],
            own_in.at[at],
            place.partner(),
        )

    def start(copies):
        for copy in copies:
            copy.start()

    total = len(chunks)
    special_at = chunks.index((0, 0))
    subs = total // 2
    lead = 2
    even_ref[...] = jnp.zeros_like(even_ref)
    odd_ref[...] = jnp.zeros_like(odd_ref)
    loads[0].wait()
    tile_ref[member] = prepare(1, True)
    loads[1].wait()
    forward(1, 0, 0)
    met()
    start(spread(0))
    start(spread_tile())
    forward(1, 1, 1)
    loads[2].wait()
    wide_table()
    lax.fori_loop(2, subs, lambda at, carry: forward(1, at, at), None)
    start(spread(1))
    prepare(0, False)
    loads[3].wait()
    lax.fori_loop(0, subs, lambda at, carry: forward(0, at, subs + at), None)

    def one(at, carry):
        spread_all(at).wait_recv()

        @pl.when(at != special_at)
        def _():
            middle(at, False)

        @pl.when(at == special_at)
        def _():
            middle(at, True)

        start([cross(at)])

        @pl.when(at + lead < total)
        def _():
            start(spread(at + lead))

        @pl.when(at == 0)
        def _():
            tile_all().wait_recv()
            half_ref[...] = jnp.sum(tile_ref[...], axis=0)
            start([far()])

        @pl.when(at >= 2)
        def _():
            join(at - 2)

        @pl.when(at >= subs)
        def _():
            back_all(at - subs).wait_recv()
            backward(1, at - subs, at - subs)

        return carry

    lax.fori_loop(0, total, one, 0)
    far().wait_recv()
    energy_ref[0, 0] = jnp.sum(half_ref[...] + far_ref[...]) / cells

    def last(at, carry):
        @pl.when(at < 2)
        def _():
            join(at + total - 2)

        back_all(at + subs).wait_recv()
        backward(0, at, at + subs)
        return carry

    lax.fori_loop(0, subs, last, 0)

    def sent(at, carry):
        for copy in (spread_all(at), back_all(at), cross(at)):
            copy.wait_send()
        return carry

    lax.fori_loop(0, total, sent, 0)
    for copy in (tile_all(), far()):
        copy.wait_send()


def combine_kernel(even_ref, odd_ref, out_ref):
    planes, rows, full_y = out_ref.shape
    half = full_y // 2
    for plane in range(planes):
        even_rows = even_ref[plane * rows : (plane + 1) * rows, :]
        odd_rows = odd_ref[plane * rows : (plane + 1) * rows, :]
        out_ref[plane, :, :half] = even_rows + odd_rows
        out_ref[plane, :, half:] = even_rows - odd_rows


def kernel_step(concentration):
    planes, rows, full_y = concentration.shape
    slabs = lax.axis_size("slab")
    sections = lax.axis_size("section")
    members = slabs * sections // 2
    full_x = rows * slabs
    full_z = planes * sections
    cells = full_x * full_y * full_z
    half = full_y // 2
    subs = half // 2 // members // kk
    width = full_x // 4
    base = np.arange(width)
    step = 2.0 * math.pi / width
    coarse = base[::row_group, None] * base[None, :] % width * step
    fine = base[:row_group, None] * base[None, :] % width * step
    dft = [f(t).astype(np.float32) for t in (coarse, fine) for f in (np.cos, np.sin)]
    twist = np.arange(4)[:, None] * base[None, :] * (2.0 * math.pi / full_x)
    twist_cos, twist_sin = np.cos(twist).astype(np.float32), np.sin(twist).astype(np.float32)
    kx = np.arange(4)[:, None] + 4 * base[None, :]
    kx = np.where(2 * kx >= full_x, kx - full_x, kx) * (2.0 * math.pi / full_x)
    wave_x = (kx * kx).astype(np.float32)
    tables = [y_tables(full_y, members * subs, parity) for parity in range(2)]
    chunks = [(1, sub) for sub in range(subs)] + [(0, sub) for sub in range(subs)]
    count = len(chunks)
    columns = planes * 2 * rows
    y_rows = np.stack([np.stack(parts) for parts in tables])
    small = [np.concatenate([rows, rows]) for rows in (wave_x, twist_cos, twist_sin)]
    coarse_cos, coarse_sin, fine_cos, fine_sin = dft
    x_rows = np.concatenate([*small, coarse_cos, coarse_sin, fine_cos, fine_sin])
    operands = [concentration, y_rows, x_rows]
    f32, bf16 = jnp.float32, jnp.bfloat16
    vmem, dma = pltpu.VMEM, pltpu.SemaphoreType.DMA
    in_vmem = pl.BlockSpec(memory_space=pltpu.VMEM)
    forth = vmem((count, members, 2 * kk, columns), f32)
    half_back = vmem((count, members, 2 * kk * planes, rows), f32)
    even, odd, energy = pl.pallas_call(
        functools.partial(step_kernel, cells, chunks),
        out_shape=(
            jax.ShapeDtypeStruct((planes * rows, half), f32),
            jax.ShapeDtypeStruct((planes * rows, half), f32),
            jax.ShapeDtypeStruct((1, 1), f32),
        ),
        in_specs=[pl.BlockSpec(memory_space=pltpu.HBM)] * len(operands),
        out_specs=(in_vmem, in_vmem, pl.BlockSpec(memory_space=pltpu.SMEM)),
        scratch_shapes=[
            vmem(concentration.shape, f32),
            vmem(y_rows.shape, f32),
            vmem(x_rows.shape, f32),
            dma((4,)),
            vmem((columns, half), bf16),
            vmem((columns, half), bf16),
            vmem((width, 2 * width), bf16),
            vmem((width, 2 * width), bf16),
            vmem((4, 2, 2 * full_z, 2 * kk, width), f32),
            vmem((4, 2, full_z, 2 * kk, width), f32),
            forth,
            forth,
            half_back,
            half_back,
            half_back,
            half_back,
            vmem((members, 8, lanes), f32),
            vmem((8, lanes), f32),
            vmem((8, lanes), f32),
            *[dma((count,))] * 6,
            dma,
            dma,
            dma,
            dma,
        ],
        compiler_params=pltpu.CompilerParams(
            vmem_limit_bytes=vmem_limit, collective_id=0, has_side_effects=True
        ),
    )(*[pltpu.with_memory_space_constraint(jnp.asarray(x), pltpu.HBM) for x in operands])
    new_field = pl.pallas_call(
        combine_kernel,
        out_shape=jax.ShapeDtypeStruct(concentration.shape, f32),
        in_specs=[in_vmem] * 2,
        out_specs=in_vmem,
        compiler_params=pltpu.CompilerParams(vmem_limit_bytes=small_limit),
    )(even, odd)
    return (new_field, energy.reshape(()))


def per_device(concentration):
    planes, rows, full_y = concentration.shape
    devices = lax.axis_size("slab") * lax.axis_size("section")
    share = full_y // 4 // devices
    fits = (
        rows == lanes
        and planes * lax.axis_size("section") == 4
        and share == 2 * kk
        and devices == 32
        and lax.axis_size("section") == 2
    )
    return kernel_step(concentration) if fits else plain_step(concentration)


def solution(mesh):
    return jax.shard_map(
        per_device,
        mesh=mesh,
        in_specs=(P("section", "slab", None),),
        out_specs=(P("section", "slab", None), P()),
        check_vma=False,
    )
```

```python
import functools
import math

import jax
import jax.numpy as jnp
import numpy as np
from jax import lax
from jax.experimental import pallas as pl
from jax.experimental.pallas import tpu as pltpu
from jax.sharding import PartitionSpec as P

time_step = 100.0
kappa_grad = 2.0
stabilizer = 8.0
highest = lax.Precision.HIGHEST


def circle(length, first_total, second_total, direction):
    first_index = jnp.arange(first_total, dtype=jnp.int32)
    second_index = jnp.arange(second_total, dtype=jnp.int32)
    turn_index = first_index[:, None] * second_index[None, :] % length
    phase_angle = turn_index.astype(jnp.float32) * (2.0 * math.pi / length)
    return (jnp.cos(phase_angle), direction * jnp.sin(phase_angle))


def contract(pattern, real_part, imag_part, table_cos, table_sin):

    def product_of(operand, matrix):
        return jnp.einsum(pattern, operand, matrix, precision=highest)

    out_real = product_of(real_part, table_cos) - product_of(imag_part, table_sin)
    out_imag = product_of(real_part, table_sin) + product_of(imag_part, table_cos)
    return (out_real, out_imag)


def real_only(pattern, real_part, imag_part, table_cos, table_sin):
    return jnp.einsum(pattern, real_part, table_cos, precision=highest) - jnp.einsum(
        pattern, imag_part, table_sin, precision=highest
    )


def rotate(real_part, imag_part, table_cos, table_sin):
    return (
        real_part * table_cos - imag_part * table_sin,
        real_part * table_sin + imag_part * table_cos,
    )


def wave_square(storage, length, permuted):
    if permuted:
        actual = storage // 128 + length // 128 * (storage % 128)
    else:
        actual = storage
    signed = jnp.where(2 * actual >= length, actual - length, actual)
    phase_angle = signed.astype(jnp.float32) * (2.0 * math.pi / length)
    return phase_angle * phase_angle


def plain_step(concentration):
    plane_count, row_count, full_y = concentration.shape
    slab_count = lax.axis_size("slab")
    section_count = lax.axis_size("section")
    full_x = row_count * slab_count
    full_z = plane_count * section_count
    y_block = full_y // slab_count
    y_half = y_block // section_count
    blocks_x = full_x // 128
    blocks_y = full_y // 128
    cell_count = full_x * full_y * full_z
    slab_at = lax.axis_index("slab")
    section_at = lax.axis_index("section")
    squared = concentration * concentration
    bulk_sum = jnp.sum(0.25 * squared * squared - 0.5 * squared)
    cubic_term = squared * concentration - concentration
    shaped_c = concentration.reshape(1, plane_count, row_count, blocks_y, 128)
    shaped_g = cubic_term.reshape(1, plane_count, row_count, blocks_y, 128)
    first_cos, first_sin = circle(blocks_y, blocks_y, blocks_y, -1.0)
    part_real, part_imag = contract("fzxab,aj->fzxjb", shaped_c, shaped_g, first_cos, first_sin)
    field_total = part_real.shape[0]
    twist_cos, twist_sin = circle(full_y, blocks_y, 128, -1.0)
    part_real, part_imag = rotate(part_real, part_imag, twist_cos, twist_sin)
    lane_cos, lane_sin = circle(128, 128, 128, -1.0)
    part_real, part_imag = contract("fzxjb,bk->fxjkz", part_real, part_imag, lane_cos, lane_sin)
    outgoing = jnp.concatenate([part_real, part_imag], 0).reshape(
        2 * field_total, row_count, slab_count, y_block * plane_count
    )
    columns = lax.all_to_all(outgoing, "slab", split_axis=2, concat_axis=1, tiled=True)
    columns = columns.reshape(2 * field_total, blocks_x, 128, y_block * plane_count)
    first_cos, first_sin = circle(blocks_x, blocks_x, blocks_x, -1.0)
    part_real, part_imag = contract(
        "fabm,aj->fmjb", columns[:field_total], columns[field_total:], first_cos, first_sin
    )
    twist_cos, twist_sin = circle(full_x, blocks_x, 128, -1.0)
    part_real, part_imag = rotate(part_real, part_imag, twist_cos, twist_sin)
    part_real, part_imag = contract("fmjb,bk->fmjk", part_real, part_imag, lane_cos, lane_sin)
    spectra_x = jnp.concatenate([part_real, part_imag], 0).reshape(
        2 * field_total, y_block, plane_count, full_x
    )
    depth_cos, depth_sin = circle(full_z, full_z, full_z, -1.0)
    own_cos = lax.dynamic_slice_in_dim(depth_cos, section_at * plane_count, plane_count, 0)
    own_sin = lax.dynamic_slice_in_dim(depth_sin, section_at * plane_count, plane_count, 0)
    term_real, term_imag = contract(
        "fyzk,zq->yfqk", spectra_x[:field_total], spectra_x[field_total:], own_cos, own_sin
    )
    spectral = lax.psum_scatter(
        jnp.concatenate([term_real, term_imag], 1), "section", scatter_dimension=0, tiled=True
    )
    storage_y = slab_at * y_block + section_at * y_half + jnp.arange(y_half, dtype=jnp.int32)
    storage_x = jnp.arange(full_x, dtype=jnp.int32)
    storage_z = jnp.arange(full_z, dtype=jnp.int32)
    wave_sq = (
        wave_square(storage_y, full_y, True)[:, None, None]
        + wave_square(storage_z, full_z, False)[None, :, None]
        + wave_square(storage_x, full_x, True)[None, None, :]
    )
    numerator = 1.0 + time_step * stabilizer * wave_sq
    denominator = numerator + time_step * kappa_grad * wave_sq * wave_sq
    keep_rate = numerator / denominator
    mix_rate = time_step * wave_sq / denominator
    new_real = keep_rate * spectral[:, 0] - mix_rate * spectral[:, 1]
    new_imag = keep_rate * spectral[:, 1] + mix_rate * spectral[:, 0]
    back_cos, back_sin = circle(full_z, full_z, full_z, 1.0)
    part_real, part_imag = contract("yqk,qz->yzk", new_real, new_imag, back_cos, back_sin)
    returning = jnp.stack([part_real, part_imag], 1)
    own_planes = lax.all_to_all(returning, "section", split_axis=2, concat_axis=0, tiled=True)
    grid_real = own_planes[:, 0].reshape(y_block, plane_count, blocks_x, 128)
    grid_imag = own_planes[:, 1].reshape(y_block, plane_count, blocks_x, 128)
    lane_cos, lane_sin = circle(128, 128, 128, 1.0)
    part_real, part_imag = contract("szjk,kb->szjb", grid_real, grid_imag, lane_cos, lane_sin)
    twist_cos, twist_sin = circle(full_x, blocks_x, 128, 1.0)
    part_real, part_imag = rotate(part_real, part_imag, twist_cos, twist_sin)
    first_cos, first_sin = circle(blocks_x, blocks_x, blocks_x, 1.0)
    part_real, part_imag = contract("szjb,ja->absz", part_real, part_imag, first_cos, first_sin)
    leaving = jnp.stack([part_real, part_imag], 0).reshape(2, full_x, 1, y_block * plane_count)
    rows_back = lax.all_to_all(leaving, "slab", split_axis=1, concat_axis=2, tiled=True)
    rows_back = rows_back.reshape(2, row_count, blocks_y, 128, plane_count)
    part_real, part_imag = contract("xjkz,kb->xjbz", rows_back[0], rows_back[1], lane_cos, lane_sin)
    twist_cos, twist_sin = circle(full_y, blocks_y, 128, 1.0)
    part_real, part_imag = rotate(
        part_real, part_imag, twist_cos[:, :, None], twist_sin[:, :, None]
    )
    first_cos, first_sin = circle(blocks_y, blocks_y, blocks_y, 1.0)
    new_field = real_only("xjbz,ja->zxab", part_real, part_imag, first_cos, first_sin)
    new_field = new_field.reshape(plane_count, row_count, full_y) / cell_count
    total_bulk = lax.psum(bulk_sum, ("section", "slab"))
    energy = total_bulk / cell_count
    return (new_field, energy)


lanes = 128
row_group = 32
groups = 8
kk = 8
vmem_limit = 48 * 1024 * 1024
small_limit = 8 * 1024 * 1024


def split(values):
    high = values.astype(jnp.bfloat16)
    low = (values - high.astype(jnp.float32)).astype(jnp.bfloat16)
    return high, low


def triple(left_parts, right_parts, dims):
    def product(left, right):
        return lax.dot_general(left, right, (dims, ((), ())), preferred_element_type=jnp.float32)

    left_high, left_low = left_parts
    right_high, right_low = right_parts
    return (
        product(left_high, right_high)
        + product(left_low, right_high)
        + product(left_high, right_low)
    )


def y_tables(full_y, devices, parity):
    half = full_y // 2
    per_part = half // 2 // devices
    slot = np.arange(half)
    device, inner = slot // (2 * per_part), slot % (2 * per_part)
    part, local = inner // per_part, inner % per_part
    wave = parity + 2 * (device * per_part + local)
    position = np.arange(half)
    turns = wave[:, None] * position[None, :] % full_y
    phase = turns * (2.0 * math.pi / full_y)
    coarse = phase[::row_group]
    offset = wave[:row_group] - wave[0]
    fine = (offset[:, None] * position[None, :] % full_y) * (2.0 * math.pi / full_y)
    fine = fine + part[:row_group, None] * (0.5 * math.pi)
    return [
        table.astype(np.float32)
        for table in (np.cos(coarse), np.sin(coarse), np.cos(fine), np.sin(fine))
    ]


def y_block(refs, block, parity, kk):
    coarse_cos, coarse_sin, fine_cos, fine_sin = refs
    cos_fine, sin_fine = fine_cos[...], fine_sin[...]
    pieces = []
    for inner in range(groups):
        at = pl.ds(block * groups + inner, 1)
        piece = coarse_cos[at, :] * cos_fine - coarse_sin[at, :] * sin_fine
        if parity == 0 and inner == 0:
            row = lax.broadcasted_iota(jnp.int32, piece.shape, 0)
            column = lax.broadcasted_iota(jnp.int32, piece.shape, 1)
            sign = 1.0 - 2.0 * (column % 2).astype(jnp.float32)
            wanted = jnp.where(block == 0, kk, -1)
            piece = jnp.where(row == wanted, sign, piece)
        pieces.append(piece)
    return jnp.concatenate(pieces, 0)


def times_unit(real, imag, quarter_turns):
    turns = quarter_turns % 4
    if turns == 0:
        return real, imag
    if turns == 1:
        return -imag, real
    if turns == 2:
        return -real, -imag
    return imag, -real


def unit_sum(parts, power, direction):
    total_real, total_imag = parts[0]
    for index in range(1, len(parts)):
        real, imag = times_unit(*parts[index], direction * power * index)
        total_real = total_real + real
        total_imag = total_imag + imag
    return total_real, total_imag


def flip(bit, wanted):
    return 1 - bit if wanted else bit


class Place:
    def __init__(self):
        self.section = lax.axis_index("section")
        self.slab = lax.axis_index("slab")
        self.upper = self.slab // 8
        depth = self.slab // 4 % 2
        self.inner = depth + self.upper - 2 * depth * self.upper
        self.bits = [self.slab % 2, self.slab // 2 % 2, 1 - self.inner, self.section]
        self.here = self.indices(self.bits)

    def indices(self, bits):
        inner = 1 - bits[2]
        depth = inner + self.upper - 2 * inner * self.upper
        low = bits[1] * 2 + bits[0]
        by_rows = bits[3] * 8 + depth * 4 + low
        by_waves = bits[3] * 8 + inner * 4 + low
        among_inner = bits[3] * 4 + low
        return by_rows, by_waves, among_inner, (bits[3], self.upper * 8 + depth * 4 + low)

    def peer(self, turn):
        return self.indices([flip(bit, turn >> at & 1) for at, bit in enumerate(self.bits)])

    def partner(self):
        return self.section, 12 - self.slab // 4 * 4 + self.slab % 4


def remote(source, target, send, receive, device):
    return pltpu.make_async_remote_copy(
        src_ref=source,
        dst_ref=target,
        send_sem=send,
        recv_sem=receive,
        device_id=device,
        device_id_type=pl.DeviceIdType.MESH,
    )


same_side = [turn for turn in range(1, 16) if not turn & 4]
other_side = [turn for turn in range(1, 16) if turn & 4]
turn_order = list(range(1, 16))
lead, lag, wait_lag = 5, 2, 6


def greet(place):
    barrier = pltpu.get_barrier_semaphore()
    devices = [place.peer(turn)[3] for turn in turn_order] + [place.partner()]
    for device in devices:
        pl.semaphore_signal(
            barrier, inc=1, device_id=device, device_id_type=pl.DeviceIdType.MESH
        )
    return lambda: pl.semaphore_wait(barrier, len(devices))


def step_kernel(cells, chunks, conc_from, y_from, x_from, *refs):
    even_ref, odd_ref, energy_ref = refs[0:3]
    (
        conc_ref, y_ref, x_ref, loaded,
        high_ref, low_ref, wide_high, wide_low, spec_ref, fil_ref,
        sent_ref, arrived_ref, own_ref, other_ref, partner_ref, returned_ref,
        tile_ref, half_ref, far_ref,
        sent_out, sent_in, other_out, other_in, own_out, own_in, tile_out, tile_in,
        half_out, half_in,
    ) = refs[3:]
    loads = [
        pltpu.make_async_copy(conc_from, conc_ref, loaded.at[0]),
        pltpu.make_async_copy(y_from.at[1], y_ref.at[1], loaded.at[1]),
        pltpu.make_async_copy(x_from, x_ref, loaded.at[2]),
        pltpu.make_async_copy(y_from.at[0], y_ref.at[0], loaded.at[3]),
    ]
    for load in loads:
        load.start()
    tables = [[y_ref.at[parity, at] for at in range(4)] for parity in range(2)]
    x_rows = x_ref.shape[0]
    short = row_group // 2
    starts = [0, 8, 16, 24, 24 + short, 24 + 2 * short, 24 + 2 * short + row_group]
    ends = starts[1:] + [x_rows]
    wx_ref, tw_cos, tw_sin, ca, sa, cb, sb = [
        x_ref.at[slice(start, end)] for start, end in zip(starts, ends)
    ]
    place = Place()
    by_rows, by_waves, among_inner, _ = place.here
    is_inner = place.inner == 1
    planes, rows, full_y = conc_ref.shape
    half = full_y // 2
    members, inner, columns = arrived_ref.shape[1:]
    items = arrived_ref.shape[0]
    width = spec_ref.shape[4]
    sections = 2
    full_z = planes * sections
    zf_local = planes * 2
    total_zf = zf_local * sections
    slabs = members // sections
    quarter = slabs // 2
    met = greet(place)

    def prepare(parity, wants_bulk):
        total = jnp.zeros((8, lanes), jnp.float32)
        for plane in range(planes):
            first = conc_ref[plane, :, :half]
            second = conc_ref[plane, :, half:]
            first_sq, second_sq = first * first, second * second
            if wants_bulk:
                bulk = 0.25 * (first_sq * first_sq + second_sq * second_sq)
                bulk = bulk - 0.5 * (first_sq + second_sq)
                bulk = jnp.sum(bulk.reshape(rows // 8, 8, half), axis=0)
                for at in range(0, half, lanes):
                    total = total + bulk[:, at : at + lanes]
            first_g = first_sq * first - first
            second_g = second_sq * second - second
            for field, (left, right) in enumerate(((first, second), (first_g, second_g))):
                mixed = left + right if parity == 0 else left - right
                high, low = split(mixed)
                at = (plane * 2 + field) * rows
                high_ref[at : at + rows, :] = high
                low_ref[at : at + rows, :] = low
        return total

    def forward(parity, sub, at):
        table = y_block(tables[parity], sub, parity, kk)
        result = triple(split(table), (high_ref[...], low_ref[...]), ((1,), (1,)))
        sent_ref[at] = result.reshape(members, inner, columns)

    def shared(item):
        return lax.rem(item, 3) == 0

    def takes(item):
        return shared(item) | is_inner

    def chunk_of(item):
        return item // 3 * 2 + jnp.where(shared(item), 0, 1)

    def slot_of(item, waves, order):
        return jnp.where(shared(item), waves, 2 * order + lax.rem(item, 3) - 1)

    def copies_out(item, turns):
        copies = []
        for turn in turns:
            _, waves, order, device = place.peer(turn)
            copies.append(
                remote(
                    sent_ref.at[chunk_of(item), slot_of(item, waves, order)],
                    arrived_ref.at[item, by_rows],
                    sent_out.at[item],
                    sent_in.at[item],
                    device,
                )
            )
        return copies

    def spread(item):
        @pl.when(shared(item) | is_inner)
        def _():
            start(copies_out(item, same_side))

        @pl.when(shared(item) | ~is_inner)
        def _():
            start(copies_out(item, other_side))

        @pl.when(takes(item))
        def _():
            slot = slot_of(item, by_waves, among_inner)
            arrived_ref[item, by_rows] = sent_ref[chunk_of(item), slot]

    def spread_tile():
        copies = []
        for turn in turn_order:
            copies.append(
                remote(
                    tile_ref.at[by_rows],
                    tile_ref.at[by_rows],
                    tile_out,
                    tile_in,
                    place.peer(turn)[3],
                )
            )
        return copies

    def wide_table():
        cos_rows, sin_rows = [], []
        cos_fine, sin_fine = cb[...], sb[...]
        for group in range(row_group // 2):
            cos_base, sin_base = ca[group : group + 1, :], sa[group : group + 1, :]
            cos_rows.append(cos_base * cos_fine - sin_base * sin_fine)
            sin_rows.append(sin_base * cos_fine + cos_base * sin_fine)
        table = jnp.concatenate([jnp.concatenate(cos_rows, 0), jnp.concatenate(sin_rows, 0)], 1)
        wide_high[...], wide_low[...] = split(table)

    def middle(item, has_extra):
        depth = 2 * kk if has_extra else kk
        chunk = chunk_of(item)
        sub = lax.rem(chunk, len(chunks) // 2)
        parity = jnp.where(chunk < len(chunks) // 2, 1, 0)
        slot = slot_of(item, by_waves, among_inner)
        base_wave = parity + 2 * kk * (sub * members + slot)
        row_iota = lax.broadcasted_iota(jnp.int32, (kk, 1), 0)
        special = None
        if has_extra:
            wanted = jnp.where(slot == 0, 0, -1)
            special = jnp.where(row_iota == wanted, 1.0, 0.0)

        def gather(section, a, part, zf):
            pieces = [
                arrived_ref[
                    item,
                    section * slabs + a * quarter + step,
                    part * kk : (part + 1) * kk,
                    zf * lanes : (zf + 1) * lanes,
                ]
                for step in range(quarter)
            ]
            return jnp.concatenate(pieces, 1)

        def put(parts, at, row):
            for j in range(4):
                real, imag = unit_sum(parts, j, -1)
                if j:
                    cos, sin = tw_cos[j : j + 1, :], tw_sin[j : j + 1, :]
                    real, imag = real * cos + imag * sin, imag * cos - real * sin
                spec_ref[j, 0, at, row : row + kk, :] = real
                spec_ref[j, 1, at, row : row + kk, :] = imag

        for section in range(sections):
            for zf in range(zf_local):
                at = section * zf_local + zf
                parts, extra = [], []
                for a in range(2):
                    real, imag = gather(section, a, 0, zf), gather(section, a, 1, zf)
                    if has_extra:
                        extra.append((imag * special, jnp.zeros_like(imag)))
                        imag = imag * (1.0 - special)
                    parts.append((real, imag))
                put(parts, at, 0)
                if has_extra:
                    put(extra, at, kk)

        weights = (wide_high[...], wide_low[...])

        def one(pair, carry):
            source = spec_ref[pl.ds(2 * pair, 2), :, :, 0:depth, :]
            raw = triple(split(source.reshape(4 * total_zf * depth, width)), weights, ((1,), (0,)))
            raw = raw.reshape(2, 2, total_zf, depth, 2 * width)
            for inside in range(2):
                j = 2 * pair + inside
                for row in range(0, depth, kk):
                    fields = []
                    for field in range(2):
                        per_z = []
                        for z in range(full_z):
                            re_part = raw[inside, 0, z * 2 + field, row : row + kk]
                            im_part = raw[inside, 1, z * 2 + field, row : row + kk]
                            per_z.append(
                                (
                                    re_part[:, :width] + im_part[:, width:],
                                    im_part[:, :width] - re_part[:, width:],
                                )
                            )
                        fields.append(per_z)
                    wave = base_wave + 2 * row_iota
                    if row:
                        wave = jnp.full_like(wave, half)
                    first = (wave == 0) | (wave == half)
                    weight = jnp.where(first, 1.0 / cells, 2.0 / cells)
                    angle = wave.astype(jnp.float32) * (2.0 * math.pi / full_y)
                    plane_sq = angle * angle + wx_ref[pl.ds(j, 1), :]
                    updated = []
                    for q in range(full_z):
                        c_real, c_imag = unit_sum(fields[0], q, -1)
                        g_real, g_imag = unit_sum(fields[1], q, -1)
                        signed = q - full_z if 2 * q >= full_z else q
                        wave_sq = plane_sq + (2.0 * math.pi * signed / full_z) ** 2
                        numerator = 1.0 + time_step * stabilizer * wave_sq
                        denominator = numerator + time_step * kappa_grad * wave_sq * wave_sq
                        inverse = weight / denominator
                        keep = numerator * inverse
                        mix = time_step * wave_sq * inverse
                        updated.append(
                            (keep * c_real - mix * g_real, keep * c_imag - mix * g_imag)
                        )
                    for z in range(full_z):
                        real, imag = unit_sum(updated, z, 1)
                        fil_ref[j, 0, z, row : row + kk, :] = real
                        fil_ref[j, 1, z, row : row + kk, :] = imag
            return carry

        lax.fori_loop(0, 2, one, 0)
        source = fil_ref[:, :, :, 0:depth, :].reshape(8 * full_z * depth, width)
        raw = triple(split(source), weights, ((1,), (0,))).reshape(4, 2, full_z, depth, 2 * width)

        def back(z, row):
            parts = []
            for j in range(4):
                re_part = raw[j, 0, z, row : row + kk]
                im_part = raw[j, 1, z, row : row + kk]
                real = re_part[:, :width] - im_part[:, width:]
                imag = re_part[:, width:] + im_part[:, :width]
                if j:
                    cos, sin = tw_cos[j : j + 1, :], tw_sin[j : j + 1, :]
                    real, imag = real * cos - imag * sin, imag * cos + real * sin
                parts.append((real, imag))
            return parts

        for z in range(full_z):
            section, plane = z // planes, z % planes
            parts = back(z, 0)
            extra = back(z, kk) if has_extra else None
            for a in range(4):
                real, imag = unit_sum(parts, a, 1)
                if has_extra:
                    extra_real, _ = unit_sum(extra, a, 1)
                    imag = imag * (1.0 - special) + extra_real * special
                target_ref = own_ref if a < 2 else other_ref
                for step in range(quarter):
                    target = section * slabs + a % 2 * quarter + step
                    piece = slice(step * lanes, (step + 1) * lanes)
                    at = plane * inner
                    target_ref[item, target, at : at + kk, :] = real[:, piece]
                    target_ref[item, target, at + kk : at + 2 * kk, :] = imag[:, piece]

    def cross(item):
        return remote(
            other_ref.at[item],
            partner_ref.at[item],
            other_out.at[item],
            other_in.at[item],
            place.partner(),
        )

    def far():
        return remote(half_ref, far_ref, half_out, half_in, place.partner())

    def join(item):
        @pl.when(takes(item))
        def _():
            cross(item).wait_recv()
            chunk, slot = chunk_of(item), slot_of(item, by_waves, among_inner)
            own_ref[item] = own_ref[item] + partner_ref[item]
            returned_ref[chunk, slot] = own_ref[item, by_rows]
            for turn in turn_order:
                rows_at, _, _, device = place.peer(turn)
                remote(
                    own_ref.at[item, rows_at],
                    returned_ref.at[chunk, slot],
                    own_out.at[item],
                    own_in.at[item],
                    device,
                ).start()

    def backward(parity, sub, chunk):
        turned = [
            returned_ref[chunk, :, plane * inner : (plane + 1) * inner, :]
            .reshape(members * inner, rows)
            .T
            for plane in range(planes)
        ]
        table = y_block(tables[parity], sub, parity, kk)
        term = triple(split(jnp.concatenate(turned, 0)), split(table), ((1,), (0,)))
        target = (even_ref, odd_ref)[parity]
        target[...] = target[...] + term

    def forth(item, count):
        return remote(
            sent_ref.at[0, 0:count],
            arrived_ref.at[item, 0:count],
            sent_out.at[item],
            sent_in.at[item],
            place.partner(),
        )

    def tile_all():
        part = tile_ref.at[0 : members - 1]
        return remote(part, part, tile_out, tile_in, place.partner())

    def home(item, count):
        return remote(
            own_ref.at[item, 0:count],
            returned_ref.at[chunk_of(item), 0:count],
            own_out.at[item],
            own_in.at[item],
            place.partner(),
        )

    def by_kind(item, act):
        for count, kind in (
            (members - 1, shared(item)),
            (len(same_side), ~shared(item) & is_inner),
            (len(other_side), ~shared(item) & ~is_inner),
        ):

            @pl.when(kind)
            def _():
                act(count)

    def wait_home(chunk):
        first = chunk // 2 * 3 + lax.rem(chunk, 2)
        by_kind(first, lambda count: home(first, count).wait_recv())

        @pl.when(lax.rem(chunk, 2) == 1)
        def _():
            by_kind(first + 1, lambda count: home(first + 1, count).wait_recv())

    def start(copies):
        for copy in copies:
            copy.start()

    total = len(chunks)
    subs = total // 2
    special_at = chunks.index((0, 0)) // 2 * 3
    even_ref[...] = jnp.zeros_like(even_ref)
    odd_ref[...] = jnp.zeros_like(odd_ref)
    loads[0].wait()
    tile_ref[by_rows] = prepare(1, True)
    loads[1].wait()
    forward(1, 0, 0)
    met()
    spread(0)
    start(spread_tile())
    forward(1, 1, 1)
    loads[2].wait()
    wide_table()
    lax.fori_loop(2, subs, lambda at, carry: forward(1, at, at), None)
    for item in range(1, lead):
        spread(item)
    prepare(0, False)
    loads[3].wait()
    lax.fori_loop(0, subs, lambda at, carry: forward(0, at, subs + at), None)

    def one(item, carry):
        @pl.when(takes(item))
        def _():
            forth(item, members - 1).wait_recv()

            @pl.when(item != special_at)
            def _():
                middle(item, False)

            @pl.when(item == special_at)
            def _():
                middle(item, True)

            cross(item).start()

        @pl.when(item + lead < items)
        def _():
            spread(item + lead)

        @pl.when(item == 0)
        def _():
            tile_all().wait_recv()
            half_ref[...] = jnp.sum(tile_ref[...], axis=0)
            far().start()

        @pl.when(item >= lag)
        def _():
            join(item - lag)

        @pl.when((item >= wait_lag) & (lax.rem(item, 3) != 1))
        def _():
            chunk = chunk_of(item - wait_lag)
            wait_home(chunk)
            backward(1, chunk, chunk)

        return carry

    lax.fori_loop(0, items, one, 0)
    far().wait_recv()
    energy_ref[0, 0] = jnp.sum(half_ref[...] + far_ref[...]) / cells

    def last(at, carry):
        @pl.when(at < lag)
        def _():
            join(at + items - lag)

        wait_home(at + subs)
        backward(0, at, at + subs)
        return carry

    lax.fori_loop(0, subs, last, 0)

    def sent(item, carry):
        by_kind(item, lambda count: forth(item, count).wait_send())

        @pl.when(takes(item))
        def _():
            home(item, members - 1).wait_send()
            cross(item).wait_send()

        return carry

    lax.fori_loop(0, items, sent, 0)
    tile_all().wait_send()
    far().wait_send()


def combine_kernel(even_ref, odd_ref, out_ref):
    planes, rows, full_y = out_ref.shape
    half = full_y // 2
    for plane in range(planes):
        even_rows = even_ref[plane * rows : (plane + 1) * rows, :]
        odd_rows = odd_ref[plane * rows : (plane + 1) * rows, :]
        out_ref[plane, :, :half] = even_rows + odd_rows
        out_ref[plane, :, half:] = even_rows - odd_rows


def kernel_step(concentration):
    planes, rows, full_y = concentration.shape
    slabs = lax.axis_size("slab")
    sections = lax.axis_size("section")
    members = slabs * sections // 2
    full_x = rows * slabs
    full_z = planes * sections
    cells = full_x * full_y * full_z
    half = full_y // 2
    subs = half // 2 // members // kk
    width = full_x // 4
    base = np.arange(width)
    step = 2.0 * math.pi / width
    coarse = base[::row_group, None] * base[None, :] % width * step
    fine = base[:row_group, None] * base[None, :] % width * step
    dft = [f(t).astype(np.float32) for t in (coarse, fine) for f in (np.cos, np.sin)]
    twist = np.arange(4)[:, None] * base[None, :] * (2.0 * math.pi / full_x)
    twist_cos, twist_sin = np.cos(twist).astype(np.float32), np.sin(twist).astype(np.float32)
    kx = np.arange(4)[:, None] + 4 * base[None, :]
    kx = np.where(2 * kx >= full_x, kx - full_x, kx) * (2.0 * math.pi / full_x)
    wave_x = (kx * kx).astype(np.float32)
    tables = [y_tables(full_y, members * subs, parity) for parity in range(2)]
    chunks = [(1, sub) for sub in range(subs)] + [(0, sub) for sub in range(subs)]
    count = len(chunks)
    items = count // 2 * 3
    columns = planes * 2 * rows
    y_rows = np.stack([np.stack(parts) for parts in tables])
    small = [np.concatenate([rows, rows]) for rows in (wave_x, twist_cos, twist_sin)]
    coarse_cos, coarse_sin, fine_cos, fine_sin = dft
    x_rows = np.concatenate([*small, coarse_cos, coarse_sin, fine_cos, fine_sin])
    operands = [concentration, y_rows, x_rows]
    f32, bf16 = jnp.float32, jnp.bfloat16
    vmem, dma = pltpu.VMEM, pltpu.SemaphoreType.DMA
    in_vmem = pl.BlockSpec(memory_space=pltpu.VMEM)
    half_back = vmem((items, members, 2 * kk * planes, rows), f32)
    even, odd, energy = pl.pallas_call(
        functools.partial(step_kernel, cells, chunks),
        out_shape=(
            jax.ShapeDtypeStruct((planes * rows, half), f32),
            jax.ShapeDtypeStruct((planes * rows, half), f32),
            jax.ShapeDtypeStruct((1, 1), f32),
        ),
        in_specs=[pl.BlockSpec(memory_space=pltpu.HBM)] * len(operands),
        out_specs=(in_vmem, in_vmem, pl.BlockSpec(memory_space=pltpu.SMEM)),
        scratch_shapes=[
            vmem(concentration.shape, f32),
            vmem(y_rows.shape, f32),
            vmem(x_rows.shape, f32),
            dma((4,)),
            vmem((columns, half), bf16),
            vmem((columns, half), bf16),
            vmem((width, 2 * width), bf16),
            vmem((width, 2 * width), bf16),
            vmem((4, 2, 2 * full_z, 2 * kk, width), f32),
            vmem((4, 2, full_z, 2 * kk, width), f32),
            vmem((count, members, 2 * kk, columns), f32),
            vmem((items, members, 2 * kk, columns), f32),
            half_back,
            half_back,
            half_back,
            vmem((count, members, 2 * kk * planes, rows), f32),
            vmem((members, 8, lanes), f32),
            vmem((8, lanes), f32),
            vmem((8, lanes), f32),
            *[dma((items,))] * 6,
            dma,
            dma,
            dma,
            dma,
        ],
        compiler_params=pltpu.CompilerParams(
            vmem_limit_bytes=vmem_limit, collective_id=0, has_side_effects=True
        ),
    )(*[pltpu.with_memory_space_constraint(jnp.asarray(x), pltpu.HBM) for x in operands])
    new_field = pl.pallas_call(
        combine_kernel,
        out_shape=jax.ShapeDtypeStruct(concentration.shape, f32),
        in_specs=[in_vmem] * 2,
        out_specs=in_vmem,
        compiler_params=pltpu.CompilerParams(vmem_limit_bytes=small_limit),
    )(even, odd)
    return (new_field, energy.reshape(()))


def per_device(concentration):
    planes, rows, full_y = concentration.shape
    devices = lax.axis_size("slab") * lax.axis_size("section")
    share = full_y // 4 // devices
    fits = (
        rows == lanes
        and planes * lax.axis_size("section") == 4
        and share == 2 * kk
        and devices == 32
        and lax.axis_size("section") == 2
    )
    return kernel_step(concentration) if fits else plain_step(concentration)


def solution(mesh):
    return jax.shard_map(
        per_device,
        mesh=mesh,
        in_specs=(P("section", "slab", None),),
        out_specs=(P("section", "slab", None), P()),
        check_vma=False,
    )
```

```python
import functools
import math

import jax
import jax.numpy as jnp
import numpy as np
from jax import lax
from jax.experimental import pallas as pl
from jax.experimental.pallas import tpu as pltpu
from jax.sharding import PartitionSpec as P

time_step = 100.0
kappa_grad = 2.0
stabilizer = 8.0
highest = lax.Precision.HIGHEST


def circle(length, first_total, second_total, direction):
    first_index = jnp.arange(first_total, dtype=jnp.int32)
    second_index = jnp.arange(second_total, dtype=jnp.int32)
    turn_index = first_index[:, None] * second_index[None, :] % length
    phase_angle = turn_index.astype(jnp.float32) * (2.0 * math.pi / length)
    return (jnp.cos(phase_angle), direction * jnp.sin(phase_angle))


def contract(pattern, real_part, imag_part, table_cos, table_sin):

    def product_of(operand, matrix):
        return jnp.einsum(pattern, operand, matrix, precision=highest)

    out_real = product_of(real_part, table_cos) - product_of(imag_part, table_sin)
    out_imag = product_of(real_part, table_sin) + product_of(imag_part, table_cos)
    return (out_real, out_imag)


def real_only(pattern, real_part, imag_part, table_cos, table_sin):
    return jnp.einsum(pattern, real_part, table_cos, precision=highest) - jnp.einsum(
        pattern, imag_part, table_sin, precision=highest
    )


def rotate(real_part, imag_part, table_cos, table_sin):
    return (
        real_part * table_cos - imag_part * table_sin,
        real_part * table_sin + imag_part * table_cos,
    )


def wave_square(storage, length, permuted):
    if permuted:
        actual = storage // 128 + length // 128 * (storage % 128)
    else:
        actual = storage
    signed = jnp.where(2 * actual >= length, actual - length, actual)
    phase_angle = signed.astype(jnp.float32) * (2.0 * math.pi / length)
    return phase_angle * phase_angle


def plain_step(concentration):
    plane_count, row_count, full_y = concentration.shape
    slab_count = lax.axis_size("slab")
    section_count = lax.axis_size("section")
    full_x = row_count * slab_count
    full_z = plane_count * section_count
    y_block = full_y // slab_count
    y_half = y_block // section_count
    blocks_x = full_x // 128
    blocks_y = full_y // 128
    cell_count = full_x * full_y * full_z
    slab_at = lax.axis_index("slab")
    section_at = lax.axis_index("section")
    squared = concentration * concentration
    bulk_sum = jnp.sum(0.25 * squared * squared - 0.5 * squared)
    cubic_term = squared * concentration - concentration
    shaped_c = concentration.reshape(1, plane_count, row_count, blocks_y, 128)
    shaped_g = cubic_term.reshape(1, plane_count, row_count, blocks_y, 128)
    first_cos, first_sin = circle(blocks_y, blocks_y, blocks_y, -1.0)
    part_real, part_imag = contract("fzxab,aj->fzxjb", shaped_c, shaped_g, first_cos, first_sin)
    field_total = part_real.shape[0]
    twist_cos, twist_sin = circle(full_y, blocks_y, 128, -1.0)
    part_real, part_imag = rotate(part_real, part_imag, twist_cos, twist_sin)
    lane_cos, lane_sin = circle(128, 128, 128, -1.0)
    part_real, part_imag = contract("fzxjb,bk->fxjkz", part_real, part_imag, lane_cos, lane_sin)
    outgoing = jnp.concatenate([part_real, part_imag], 0).reshape(
        2 * field_total, row_count, slab_count, y_block * plane_count
    )
    columns = lax.all_to_all(outgoing, "slab", split_axis=2, concat_axis=1, tiled=True)
    columns = columns.reshape(2 * field_total, blocks_x, 128, y_block * plane_count)
    first_cos, first_sin = circle(blocks_x, blocks_x, blocks_x, -1.0)
    part_real, part_imag = contract(
        "fabm,aj->fmjb", columns[:field_total], columns[field_total:], first_cos, first_sin
    )
    twist_cos, twist_sin = circle(full_x, blocks_x, 128, -1.0)
    part_real, part_imag = rotate(part_real, part_imag, twist_cos, twist_sin)
    part_real, part_imag = contract("fmjb,bk->fmjk", part_real, part_imag, lane_cos, lane_sin)
    spectra_x = jnp.concatenate([part_real, part_imag], 0).reshape(
        2 * field_total, y_block, plane_count, full_x
    )
    depth_cos, depth_sin = circle(full_z, full_z, full_z, -1.0)
    own_cos = lax.dynamic_slice_in_dim(depth_cos, section_at * plane_count, plane_count, 0)
    own_sin = lax.dynamic_slice_in_dim(depth_sin, section_at * plane_count, plane_count, 0)
    term_real, term_imag = contract(
        "fyzk,zq->yfqk", spectra_x[:field_total], spectra_x[field_total:], own_cos, own_sin
    )
    spectral = lax.psum_scatter(
        jnp.concatenate([term_real, term_imag], 1), "section", scatter_dimension=0, tiled=True
    )
    storage_y = slab_at * y_block + section_at * y_half + jnp.arange(y_half, dtype=jnp.int32)
    storage_x = jnp.arange(full_x, dtype=jnp.int32)
    storage_z = jnp.arange(full_z, dtype=jnp.int32)
    wave_sq = (
        wave_square(storage_y, full_y, True)[:, None, None]
        + wave_square(storage_z, full_z, False)[None, :, None]
        + wave_square(storage_x, full_x, True)[None, None, :]
    )
    numerator = 1.0 + time_step * stabilizer * wave_sq
    denominator = numerator + time_step * kappa_grad * wave_sq * wave_sq
    keep_rate = numerator / denominator
    mix_rate = time_step * wave_sq / denominator
    new_real = keep_rate * spectral[:, 0] - mix_rate * spectral[:, 1]
    new_imag = keep_rate * spectral[:, 1] + mix_rate * spectral[:, 0]
    back_cos, back_sin = circle(full_z, full_z, full_z, 1.0)
    part_real, part_imag = contract("yqk,qz->yzk", new_real, new_imag, back_cos, back_sin)
    returning = jnp.stack([part_real, part_imag], 1)
    own_planes = lax.all_to_all(returning, "section", split_axis=2, concat_axis=0, tiled=True)
    grid_real = own_planes[:, 0].reshape(y_block, plane_count, blocks_x, 128)
    grid_imag = own_planes[:, 1].reshape(y_block, plane_count, blocks_x, 128)
    lane_cos, lane_sin = circle(128, 128, 128, 1.0)
    part_real, part_imag = contract("szjk,kb->szjb", grid_real, grid_imag, lane_cos, lane_sin)
    twist_cos, twist_sin = circle(full_x, blocks_x, 128, 1.0)
    part_real, part_imag = rotate(part_real, part_imag, twist_cos, twist_sin)
    first_cos, first_sin = circle(blocks_x, blocks_x, blocks_x, 1.0)
    part_real, part_imag = contract("szjb,ja->absz", part_real, part_imag, first_cos, first_sin)
    leaving = jnp.stack([part_real, part_imag], 0).reshape(2, full_x, 1, y_block * plane_count)
    rows_back = lax.all_to_all(leaving, "slab", split_axis=1, concat_axis=2, tiled=True)
    rows_back = rows_back.reshape(2, row_count, blocks_y, 128, plane_count)
    part_real, part_imag = contract("xjkz,kb->xjbz", rows_back[0], rows_back[1], lane_cos, lane_sin)
    twist_cos, twist_sin = circle(full_y, blocks_y, 128, 1.0)
    part_real, part_imag = rotate(
        part_real, part_imag, twist_cos[:, :, None], twist_sin[:, :, None]
    )
    first_cos, first_sin = circle(blocks_y, blocks_y, blocks_y, 1.0)
    new_field = real_only("xjbz,ja->zxab", part_real, part_imag, first_cos, first_sin)
    new_field = new_field.reshape(plane_count, row_count, full_y) / cell_count
    total_bulk = lax.psum(bulk_sum, ("section", "slab"))
    energy = total_bulk / cell_count
    return (new_field, energy)


lanes = 128
row_group = 32
groups = 8
kk = 8
vmem_limit = 48 * 1024 * 1024
small_limit = 8 * 1024 * 1024


def split(values):
    high = values.astype(jnp.bfloat16)
    low = (values - high.astype(jnp.float32)).astype(jnp.bfloat16)
    return high, low


def triple(left_parts, right_parts, dims):
    def product(left, right):
        return lax.dot_general(left, right, (dims, ((), ())), preferred_element_type=jnp.float32)

    left_high, left_low = left_parts
    right_high, right_low = right_parts
    return (
        product(left_high, right_high)
        + product(left_low, right_high)
        + product(left_high, right_low)
    )


def y_tables(full_y, devices, parity):
    half = full_y // 2
    per_part = half // 2 // devices
    slot = np.arange(half)
    device, inner = slot // (2 * per_part), slot % (2 * per_part)
    part, local = inner // per_part, inner % per_part
    wave = parity + 2 * (device * per_part + local)
    position = np.arange(half)
    turns = wave[:, None] * position[None, :] % full_y
    phase = turns * (2.0 * math.pi / full_y)
    coarse = phase[::row_group]
    offset = wave[:row_group] - wave[0]
    fine = (offset[:, None] * position[None, :] % full_y) * (2.0 * math.pi / full_y)
    fine = fine + part[:row_group, None] * (0.5 * math.pi)
    return [
        table.astype(np.float32)
        for table in (np.cos(coarse), np.sin(coarse), np.cos(fine), np.sin(fine))
    ]


def y_block(refs, block, parity, kk):
    coarse_cos, coarse_sin, fine_cos, fine_sin = refs
    cos_fine, sin_fine = fine_cos[...], fine_sin[...]
    pieces = []
    for inner in range(groups):
        at = pl.ds(block * groups + inner, 1)
        piece = coarse_cos[at, :] * cos_fine - coarse_sin[at, :] * sin_fine
        if parity == 0 and inner == 0:
            row = lax.broadcasted_iota(jnp.int32, piece.shape, 0)
            column = lax.broadcasted_iota(jnp.int32, piece.shape, 1)
            sign = 1.0 - 2.0 * (column % 2).astype(jnp.float32)
            wanted = jnp.where(block == 0, kk, -1)
            piece = jnp.where(row == wanted, sign, piece)
        pieces.append(piece)
    return jnp.concatenate(pieces, 0)


def times_unit(real, imag, quarter_turns):
    turns = quarter_turns % 4
    if turns == 0:
        return real, imag
    if turns == 1:
        return -imag, real
    if turns == 2:
        return -real, -imag
    return imag, -real


def unit_sum(parts, power, direction):
    total_real, total_imag = parts[0]
    for index in range(1, len(parts)):
        real, imag = times_unit(*parts[index], direction * power * index)
        total_real = total_real + real
        total_imag = total_imag + imag
    return total_real, total_imag


def flip(bit, wanted):
    return 1 - bit if wanted else bit


class Place:
    def __init__(self):
        self.section = lax.axis_index("section")
        self.slab = lax.axis_index("slab")
        self.upper = self.slab // 8
        depth = self.slab // 4 % 2
        self.inner = depth + self.upper - 2 * depth * self.upper
        self.bits = [self.slab % 2, self.slab // 2 % 2, 1 - self.inner, self.section]
        self.here = self.indices(self.bits)

    def indices(self, bits):
        inner = 1 - bits[2]
        depth = inner + self.upper - 2 * inner * self.upper
        low = bits[1] * 2 + bits[0]
        by_rows = bits[3] * 8 + depth * 4 + low
        by_waves = bits[3] * 8 + inner * 4 + low
        among_inner = bits[3] * 4 + low
        return by_rows, by_waves, among_inner, (bits[3], self.upper * 8 + depth * 4 + low)

    def peer(self, turn):
        return self.indices([flip(bit, turn >> at & 1) for at, bit in enumerate(self.bits)])

    def partner(self):
        return self.section, 12 - self.slab // 4 * 4 + self.slab % 4


def remote(source, target, send, receive, device):
    return pltpu.make_async_remote_copy(
        src_ref=source,
        dst_ref=target,
        send_sem=send,
        recv_sem=receive,
        device_id=device,
        device_id_type=pl.DeviceIdType.MESH,
    )


same_side = [8, 2, 10, 1, 9, 3, 11]
other_side = [4, 12, 6, 14, 5, 13, 7, 15]
turn_order = [4, 8, 6, 2, 12, 10, 5, 1, 14, 9, 13, 3, 7, 11, 15]
lead, lag, wait_lag = 4, 2, 6


def greet(place):
    barrier = pltpu.get_barrier_semaphore()
    devices = [place.peer(turn)[3] for turn in turn_order] + [place.partner()]
    for device in devices:
        pl.semaphore_signal(
            barrier, inc=1, device_id=device, device_id_type=pl.DeviceIdType.MESH
        )
    return lambda: pl.semaphore_wait(barrier, len(devices))


def step_kernel(cells, chunks, conc_from, y_from, x_from, *refs):
    even_ref, odd_ref, energy_ref = refs[0:3]
    (
        conc_ref, y_ref, x_ref, loaded,
        high_ref, low_ref, wide_high, wide_low, spec_ref, fil_ref,
        sent_ref, arrived_ref, own_ref, other_ref, partner_ref, returned_ref,
        tile_ref, half_ref, far_ref,
        sent_out, sent_in, other_out, other_in, own_out, own_in, tile_out, tile_in,
        half_out, half_in,
    ) = refs[3:]
    loads = [
        pltpu.make_async_copy(conc_from.at[0], conc_ref.at[0], loaded.at[0]),
        pltpu.make_async_copy(conc_from.at[1], conc_ref.at[1], loaded.at[4]),
        pltpu.make_async_copy(y_from.at[1], y_ref.at[1], loaded.at[1]),
        pltpu.make_async_copy(x_from, x_ref, loaded.at[2]),
        pltpu.make_async_copy(y_from.at[0], y_ref.at[0], loaded.at[3]),
    ]
    for load in loads:
        load.start()
    tables = [[y_ref.at[parity, at] for at in range(4)] for parity in range(2)]
    x_rows = x_ref.shape[0]
    short = row_group // 2
    starts = [0, 8, 16, 24, 24 + short, 24 + 2 * short, 24 + 2 * short + row_group]
    ends = starts[1:] + [x_rows]
    wx_ref, tw_cos, tw_sin, ca, sa, cb, sb = [
        x_ref.at[slice(start, end)] for start, end in zip(starts, ends)
    ]
    place = Place()
    by_rows, by_waves, among_inner, _ = place.here
    is_inner = place.inner == 1
    planes, rows, full_y = conc_ref.shape
    half = full_y // 2
    members, inner, columns = arrived_ref.shape[1:]
    items = arrived_ref.shape[0]
    width = spec_ref.shape[4]
    sections = 2
    full_z = planes * sections
    zf_local = planes * 2
    total_zf = zf_local * sections
    slabs = members // sections
    quarter = slabs // 2
    met = greet(place)

    def prepare(parity, wants_bulk, arriving=()):
        total = jnp.zeros((8, lanes), jnp.float32)
        for plane in range(planes):
            for load in arriving[plane : plane + 1]:
                load.wait()
            first = conc_ref[plane, :, :half]
            second = conc_ref[plane, :, half:]
            first_sq, second_sq = first * first, second * second
            if wants_bulk:
                bulk = 0.25 * (first_sq * first_sq + second_sq * second_sq)
                bulk = bulk - 0.5 * (first_sq + second_sq)
                bulk = jnp.sum(bulk.reshape(rows // 8, 8, half), axis=0)
                for at in range(0, half, lanes):
                    total = total + bulk[:, at : at + lanes]
            first_g = first_sq * first - first
            second_g = second_sq * second - second
            for field, (left, right) in enumerate(((first, second), (first_g, second_g))):
                mixed = left + right if parity == 0 else left - right
                high, low = split(mixed)
                at = (plane * 2 + field) * rows
                high_ref[at : at + rows, :] = high
                low_ref[at : at + rows, :] = low
        return total

    def forward(parity, sub, at):
        table = y_block(tables[parity], sub, parity, kk)
        result = triple(split(table), (high_ref[...], low_ref[...]), ((1,), (1,)))
        sent_ref[at] = result.reshape(members, inner, columns)

    def shared(item):
        return lax.rem(item, 3) == 0

    def takes(item):
        return shared(item) | is_inner

    def chunk_of(item):
        return item // 3 * 2 + jnp.where(shared(item), 0, 1)

    def slot_of(item, waves, order):
        return jnp.where(shared(item), waves, 2 * order + lax.rem(item, 3) - 1)

    def copies_out(item, turns):
        copies = []
        for turn in turns:
            _, waves, order, device = place.peer(turn)
            copies.append(
                remote(
                    sent_ref.at[chunk_of(item), slot_of(item, waves, order)],
                    arrived_ref.at[item, by_rows],
                    sent_out.at[item],
                    sent_in.at[item],
                    device,
                )
            )
        return copies

    def spread(item):
        @pl.when(shared(item))
        def _():
            start(copies_out(item, turn_order))

        @pl.when(~shared(item) & is_inner)
        def _():
            start(copies_out(item, same_side))

        @pl.when(~shared(item) & ~is_inner)
        def _():
            start(copies_out(item, other_side))

        @pl.when(takes(item))
        def _():
            slot = slot_of(item, by_waves, among_inner)
            arrived_ref[item, by_rows] = sent_ref[chunk_of(item), slot]

    def spread_tile():
        copies = []
        for turn in turn_order:
            copies.append(
                remote(
                    tile_ref.at[by_rows],
                    tile_ref.at[by_rows],
                    tile_out,
                    tile_in,
                    place.peer(turn)[3],
                )
            )
        return copies

    def wide_table():
        cos_rows, sin_rows = [], []
        cos_fine, sin_fine = cb[...], sb[...]
        for group in range(row_group // 2):
            cos_base, sin_base = ca[group : group + 1, :], sa[group : group + 1, :]
            cos_rows.append(cos_base * cos_fine - sin_base * sin_fine)
            sin_rows.append(sin_base * cos_fine + cos_base * sin_fine)
        table = jnp.concatenate([jnp.concatenate(cos_rows, 0), jnp.concatenate(sin_rows, 0)], 1)
        wide_high[...], wide_low[...] = split(table)

    def middle(item, has_extra):
        depth = 2 * kk if has_extra else kk
        chunk = chunk_of(item)
        sub = lax.rem(chunk, len(chunks) // 2)
        parity = jnp.where(chunk < len(chunks) // 2, 1, 0)
        slot = slot_of(item, by_waves, among_inner)
        base_wave = parity + 2 * kk * (sub * members + slot)
        row_iota = lax.broadcasted_iota(jnp.int32, (kk, 1), 0)
        special = None
        if has_extra:
            wanted = jnp.where(slot == 0, 0, -1)
            special = jnp.where(row_iota == wanted, 1.0, 0.0)

        def gather(section, a, part, zf):
            pieces = [
                arrived_ref[
                    item,
                    section * slabs + a * quarter + step,
                    part * kk : (part + 1) * kk,
                    zf * lanes : (zf + 1) * lanes,
                ]
                for step in range(quarter)
            ]
            return jnp.concatenate(pieces, 1)

        def put(parts, at, row):
            for j in range(4):
                real, imag = unit_sum(parts, j, -1)
                if j:
                    cos, sin = tw_cos[j : j + 1, :], tw_sin[j : j + 1, :]
                    real, imag = real * cos + imag * sin, imag * cos - real * sin
                spec_ref[j, 0, at, row : row + kk, :] = real
                spec_ref[j, 1, at, row : row + kk, :] = imag

        for section in range(sections):
            for zf in range(zf_local):
                at = section * zf_local + zf
                parts, extra = [], []
                for a in range(2):
                    real, imag = gather(section, a, 0, zf), gather(section, a, 1, zf)
                    if has_extra:
                        extra.append((imag * special, jnp.zeros_like(imag)))
                        imag = imag * (1.0 - special)
                    parts.append((real, imag))
                put(parts, at, 0)
                if has_extra:
                    put(extra, at, kk)

        weights = (wide_high[...], wide_low[...])

        def one(pair, carry):
            source = spec_ref[pl.ds(2 * pair, 2), :, :, 0:depth, :]
            raw = triple(split(source.reshape(4 * total_zf * depth, width)), weights, ((1,), (0,)))
            raw = raw.reshape(2, 2, total_zf, depth, 2 * width)
            for inside in range(2):
                j = 2 * pair + inside
                for row in range(0, depth, kk):
                    fields = []
                    for field in range(2):
                        per_z = []
                        for z in range(full_z):
                            re_part = raw[inside, 0, z * 2 + field, row : row + kk]
                            im_part = raw[inside, 1, z * 2 + field, row : row + kk]
                            per_z.append(
                                (
                                    re_part[:, :width] + im_part[:, width:],
                                    im_part[:, :width] - re_part[:, width:],
                                )
                            )
                        fields.append(per_z)
                    wave = base_wave + 2 * row_iota
                    if row:
                        wave = jnp.full_like(wave, half)
                    first = (wave == 0) | (wave == half)
                    weight = jnp.where(first, 1.0 / cells, 2.0 / cells)
                    angle = wave.astype(jnp.float32) * (2.0 * math.pi / full_y)
                    plane_sq = angle * angle + wx_ref[pl.ds(j, 1), :]
                    updated = []
                    for q in range(full_z):
                        c_real, c_imag = unit_sum(fields[0], q, -1)
                        g_real, g_imag = unit_sum(fields[1], q, -1)
                        signed = q - full_z if 2 * q >= full_z else q
                        wave_sq = plane_sq + (2.0 * math.pi * signed / full_z) ** 2
                        numerator = 1.0 + time_step * stabilizer * wave_sq
                        denominator = numerator + time_step * kappa_grad * wave_sq * wave_sq
                        inverse = weight / denominator
                        keep = numerator * inverse
                        mix = time_step * wave_sq * inverse
                        updated.append(
                            (keep * c_real - mix * g_real, keep * c_imag - mix * g_imag)
                        )
                    for z in range(full_z):
                        real, imag = unit_sum(updated, z, 1)
                        fil_ref[j, 0, z, row : row + kk, :] = real
                        fil_ref[j, 1, z, row : row + kk, :] = imag
            return carry

        lax.fori_loop(0, 2, one, 0)
        source = fil_ref[:, :, :, 0:depth, :].reshape(8 * full_z * depth, width)
        raw = triple(split(source), weights, ((1,), (0,))).reshape(4, 2, full_z, depth, 2 * width)

        def back(z, row):
            parts = []
            for j in range(4):
                re_part = raw[j, 0, z, row : row + kk]
                im_part = raw[j, 1, z, row : row + kk]
                real = re_part[:, :width] - im_part[:, width:]
                imag = re_part[:, width:] + im_part[:, :width]
                if j:
                    cos, sin = tw_cos[j : j + 1, :], tw_sin[j : j + 1, :]
                    real, imag = real * cos - imag * sin, imag * cos + real * sin
                parts.append((real, imag))
            return parts

        for z in range(full_z):
            section, plane = z // planes, z % planes
            parts = back(z, 0)
            extra = back(z, kk) if has_extra else None
            for a in range(4):
                real, imag = unit_sum(parts, a, 1)
                if has_extra:
                    extra_real, _ = unit_sum(extra, a, 1)
                    imag = imag * (1.0 - special) + extra_real * special
                target_ref = own_ref if a < 2 else other_ref
                for step in range(quarter):
                    target = section * slabs + a % 2 * quarter + step
                    piece = slice(step * lanes, (step + 1) * lanes)
                    at = plane * inner
                    target_ref[item, target, at : at + kk, :] = real[:, piece]
                    target_ref[item, target, at + kk : at + 2 * kk, :] = imag[:, piece]

    def cross(item):
        return remote(
            other_ref.at[item],
            partner_ref.at[item],
            other_out.at[item],
            other_in.at[item],
            place.partner(),
        )

    def far():
        return remote(half_ref, far_ref, half_out, half_in, place.partner())

    def join(item):
        @pl.when(takes(item))
        def _():
            cross(item).wait_recv()
            chunk, slot = chunk_of(item), slot_of(item, by_waves, among_inner)
            own_ref[item] = own_ref[item] + partner_ref[item]
            returned_ref[chunk, slot] = own_ref[item, by_rows]
            for turn in turn_order:
                rows_at, _, _, device = place.peer(turn)
                remote(
                    own_ref.at[item, rows_at],
                    returned_ref.at[chunk, slot],
                    own_out.at[item],
                    own_in.at[item],
                    device,
                ).start()

    def backward(parity, sub, chunk):
        turned = [
            returned_ref[chunk, :, plane * inner : (plane + 1) * inner, :]
            .reshape(members * inner, rows)
            .T
            for plane in range(planes)
        ]
        table = y_block(tables[parity], sub, parity, kk)
        term = triple(split(jnp.concatenate(turned, 0)), split(table), ((1,), (0,)))
        target = (even_ref, odd_ref)[parity]
        target[...] = target[...] + term

    def forth(item, count):
        return remote(
            sent_ref.at[0, 0:count],
            arrived_ref.at[item, 0:count],
            sent_out.at[item],
            sent_in.at[item],
            place.partner(),
        )

    def tile_all():
        part = tile_ref.at[0 : members - 1]
        return remote(part, part, tile_out, tile_in, place.partner())

    def home(item, count):
        return remote(
            own_ref.at[item, 0:count],
            returned_ref.at[chunk_of(item), 0:count],
            own_out.at[item],
            own_in.at[item],
            place.partner(),
        )

    def by_kind(item, act):
        for count, kind in (
            (members - 1, shared(item)),
            (len(same_side), ~shared(item) & is_inner),
            (len(other_side), ~shared(item) & ~is_inner),
        ):

            @pl.when(kind)
            def _():
                act(count)

    def wait_home(chunk):
        first = chunk // 2 * 3 + lax.rem(chunk, 2)
        by_kind(first, lambda count: home(first, count).wait_recv())

        @pl.when(lax.rem(chunk, 2) == 1)
        def _():
            by_kind(first + 1, lambda count: home(first + 1, count).wait_recv())

    def start(copies):
        for copy in copies:
            copy.start()

    total = len(chunks)
    subs = total // 2
    special_at = chunks.index((0, 0)) // 2 * 3
    even_ref[...] = jnp.zeros_like(even_ref)
    odd_ref[...] = jnp.zeros_like(odd_ref)
    prepare(1, False, loads)
    loads[2].wait()
    forward(1, 0, 0)
    met()
    spread(0)
    forward(1, 1, 1)
    loads[3].wait()
    wide_table()
    lax.fori_loop(2, subs, lambda at, carry: forward(1, at, at), None)
    spread(1)
    tile_ref[by_rows] = prepare(0, True)
    start(spread_tile())
    loads[4].wait()
    lax.fori_loop(0, subs, lambda at, carry: forward(0, at, subs + at), None)

    for item in range(2, lead):
        spread(item)

    def one(item, carry):
        @pl.when(takes(item))
        def _():
            forth(item, members - 1).wait_recv()

        @pl.when(item + lead < items)
        def _():
            spread(item + lead)

        @pl.when(takes(item))
        def _():
            @pl.when(item != special_at)
            def _():
                middle(item, False)

            @pl.when(item == special_at)
            def _():
                middle(item, True)

            cross(item).start()

        @pl.when(item == 0)
        def _():
            tile_all().wait_recv()
            half_ref[...] = jnp.sum(tile_ref[...], axis=0)
            far().start()

        @pl.when(item >= lag)
        def _():
            join(item - lag)

        @pl.when((item >= wait_lag) & (lax.rem(item, 3) != 1))
        def _():
            chunk = chunk_of(item - wait_lag)
            wait_home(chunk)
            backward(1, chunk, chunk)

        return carry

    lax.fori_loop(0, items, one, 0)
    far().wait_recv()
    energy_ref[0, 0] = jnp.sum(half_ref[...] + far_ref[...]) / cells

    def last(at, carry):
        @pl.when(at < lag)
        def _():
            join(at + items - lag)

        wait_home(at + subs)
        backward(0, at, at + subs)
        return carry

    lax.fori_loop(0, subs, last, 0)

    def sent(item, carry):
        by_kind(item, lambda count: forth(item, count).wait_send())

        @pl.when(takes(item))
        def _():
            home(item, members - 1).wait_send()
            cross(item).wait_send()

        return carry

    lax.fori_loop(0, items, sent, 0)
    tile_all().wait_send()
    far().wait_send()


def combine_kernel(even_ref, odd_ref, out_to, out_ref, stored):
    planes, rows, full_y = out_ref.shape
    half = full_y // 2
    step = rows // stored.shape[1]
    stores = []
    for plane in range(planes):
        for part in range(stored.shape[1]):
            here = slice(part * step, (part + 1) * step)
            at = slice(plane * rows + part * step, plane * rows + (part + 1) * step)
            even_rows, odd_rows = even_ref[at, :], odd_ref[at, :]
            out_ref[plane, here, :half] = even_rows + odd_rows
            out_ref[plane, here, half:] = even_rows - odd_rows
            store = pltpu.make_async_copy(
                out_ref.at[plane, here], out_to.at[plane, here], stored.at[plane, part]
            )
            store.start()
            stores.append(store)
    for store in stores:
        store.wait()


def kernel_step(concentration):
    planes, rows, full_y = concentration.shape
    slabs = lax.axis_size("slab")
    sections = lax.axis_size("section")
    members = slabs * sections // 2
    full_x = rows * slabs
    full_z = planes * sections
    cells = full_x * full_y * full_z
    half = full_y // 2
    subs = half // 2 // members // kk
    width = full_x // 4
    base = np.arange(width)
    step = 2.0 * math.pi / width
    coarse = base[::row_group, None] * base[None, :] % width * step
    fine = base[:row_group, None] * base[None, :] % width * step
    dft = [f(t).astype(np.float32) for t in (coarse, fine) for f in (np.cos, np.sin)]
    twist = np.arange(4)[:, None] * base[None, :] * (2.0 * math.pi / full_x)
    twist_cos, twist_sin = np.cos(twist).astype(np.float32), np.sin(twist).astype(np.float32)
    kx = np.arange(4)[:, None] + 4 * base[None, :]
    kx = np.where(2 * kx >= full_x, kx - full_x, kx) * (2.0 * math.pi / full_x)
    wave_x = (kx * kx).astype(np.float32)
    tables = [y_tables(full_y, members * subs, parity) for parity in range(2)]
    chunks = [(1, sub) for sub in range(subs)] + [(0, sub) for sub in range(subs)]
    count = len(chunks)
    items = count // 2 * 3
    columns = planes * 2 * rows
    y_rows = np.stack([np.stack(parts) for parts in tables])
    small = [np.concatenate([rows, rows]) for rows in (wave_x, twist_cos, twist_sin)]
    coarse_cos, coarse_sin, fine_cos, fine_sin = dft
    x_rows = np.concatenate([*small, coarse_cos, coarse_sin, fine_cos, fine_sin])
    operands = [concentration, y_rows, x_rows]
    f32, bf16 = jnp.float32, jnp.bfloat16
    vmem, dma = pltpu.VMEM, pltpu.SemaphoreType.DMA
    in_vmem = pl.BlockSpec(memory_space=pltpu.VMEM)
    half_back = vmem((items, members, 2 * kk * planes, rows), f32)
    even, odd, energy = pl.pallas_call(
        functools.partial(step_kernel, cells, chunks),
        out_shape=(
            jax.ShapeDtypeStruct((planes * rows, half), f32),
            jax.ShapeDtypeStruct((planes * rows, half), f32),
            jax.ShapeDtypeStruct((1, 1), f32),
        ),
        in_specs=[pl.BlockSpec(memory_space=pltpu.HBM)] * len(operands),
        out_specs=(in_vmem, in_vmem, pl.BlockSpec(memory_space=pltpu.SMEM)),
        scratch_shapes=[
            vmem(concentration.shape, f32),
            vmem(y_rows.shape, f32),
            vmem(x_rows.shape, f32),
            dma((5,)),
            vmem((columns, half), bf16),
            vmem((columns, half), bf16),
            vmem((width, 2 * width), bf16),
            vmem((width, 2 * width), bf16),
            vmem((4, 2, 2 * full_z, 2 * kk, width), f32),
            vmem((4, 2, full_z, 2 * kk, width), f32),
            vmem((count, members, 2 * kk, columns), f32),
            vmem((items, members, 2 * kk, columns), f32),
            half_back,
            half_back,
            half_back,
            vmem((count, members, 2 * kk * planes, rows), f32),
            vmem((members, 8, lanes), f32),
            vmem((8, lanes), f32),
            vmem((8, lanes), f32),
            *[dma((items,))] * 6,
            dma,
            dma,
            dma,
            dma,
        ],
        compiler_params=pltpu.CompilerParams(
            vmem_limit_bytes=vmem_limit, collective_id=0, has_side_effects=True
        ),
    )(*[pltpu.with_memory_space_constraint(jnp.asarray(x), pltpu.HBM) for x in operands])
    new_field = pl.pallas_call(
        combine_kernel,
        out_shape=jax.ShapeDtypeStruct(concentration.shape, f32),
        in_specs=[in_vmem] * 2,
        out_specs=pl.BlockSpec(memory_space=pltpu.HBM),
        scratch_shapes=[vmem(concentration.shape, f32), dma((planes, 2))],
        compiler_params=pltpu.CompilerParams(vmem_limit_bytes=small_limit),
    )(even, odd)
    return (new_field, energy.reshape(()))


def per_device(concentration):
    planes, rows, full_y = concentration.shape
    devices = lax.axis_size("slab") * lax.axis_size("section")
    share = full_y // 4 // devices
    fits = (
        rows == lanes
        and planes * lax.axis_size("section") == 4
        and share == 2 * kk
        and devices == 32
        and lax.axis_size("section") == 2
    )
    return kernel_step(concentration) if fits else plain_step(concentration)


def solution(mesh):
    return jax.shard_map(
        per_device,
        mesh=mesh,
        in_specs=(P("section", "slab", None),),
        out_specs=(P("section", "slab", None), P()),
        check_vma=False,
    )
```

```python
import functools
import math

import jax
import jax.numpy as jnp
import numpy as np
from jax import lax
from jax.experimental import pallas as pl
from jax.experimental.pallas import tpu as pltpu
from jax.sharding import PartitionSpec as P

time_step = 100.0
kappa_grad = 2.0
stabilizer = 8.0
highest = lax.Precision.HIGHEST


def circle(length, first_total, second_total, direction):
    first_index = jnp.arange(first_total, dtype=jnp.int32)
    second_index = jnp.arange(second_total, dtype=jnp.int32)
    turn_index = first_index[:, None] * second_index[None, :] % length
    phase_angle = turn_index.astype(jnp.float32) * (2.0 * math.pi / length)
    return (jnp.cos(phase_angle), direction * jnp.sin(phase_angle))


def contract(pattern, real_part, imag_part, table_cos, table_sin):

    def product_of(operand, matrix):
        return jnp.einsum(pattern, operand, matrix, precision=highest)

    out_real = product_of(real_part, table_cos) - product_of(imag_part, table_sin)
    out_imag = product_of(real_part, table_sin) + product_of(imag_part, table_cos)
    return (out_real, out_imag)


def real_only(pattern, real_part, imag_part, table_cos, table_sin):
    return jnp.einsum(pattern, real_part, table_cos, precision=highest) - jnp.einsum(
        pattern, imag_part, table_sin, precision=highest
    )


def rotate(real_part, imag_part, table_cos, table_sin):
    return (
        real_part * table_cos - imag_part * table_sin,
        real_part * table_sin + imag_part * table_cos,
    )


def wave_square(storage, length, permuted):
    if permuted:
        actual = storage // 128 + length // 128 * (storage % 128)
    else:
        actual = storage
    signed = jnp.where(2 * actual >= length, actual - length, actual)
    phase_angle = signed.astype(jnp.float32) * (2.0 * math.pi / length)
    return phase_angle * phase_angle


def plain_step(concentration):
    plane_count, row_count, full_y = concentration.shape
    slab_count = lax.axis_size("slab")
    section_count = lax.axis_size("section")
    full_x = row_count * slab_count
    full_z = plane_count * section_count
    y_block = full_y // slab_count
    y_half = y_block // section_count
    blocks_x = full_x // 128
    blocks_y = full_y // 128
    cell_count = full_x * full_y * full_z
    slab_at = lax.axis_index("slab")
    section_at = lax.axis_index("section")
    squared = concentration * concentration
    bulk_sum = jnp.sum(0.25 * squared * squared - 0.5 * squared)
    cubic_term = squared * concentration - concentration
    shaped_c = concentration.reshape(1, plane_count, row_count, blocks_y, 128)
    shaped_g = cubic_term.reshape(1, plane_count, row_count, blocks_y, 128)
    first_cos, first_sin = circle(blocks_y, blocks_y, blocks_y, -1.0)
    part_real, part_imag = contract("fzxab,aj->fzxjb", shaped_c, shaped_g, first_cos, first_sin)
    field_total = part_real.shape[0]
    twist_cos, twist_sin = circle(full_y, blocks_y, 128, -1.0)
    part_real, part_imag = rotate(part_real, part_imag, twist_cos, twist_sin)
    lane_cos, lane_sin = circle(128, 128, 128, -1.0)
    part_real, part_imag = contract("fzxjb,bk->fxjkz", part_real, part_imag, lane_cos, lane_sin)
    outgoing = jnp.concatenate([part_real, part_imag], 0).reshape(
        2 * field_total, row_count, slab_count, y_block * plane_count
    )
    columns = lax.all_to_all(outgoing, "slab", split_axis=2, concat_axis=1, tiled=True)
    columns = columns.reshape(2 * field_total, blocks_x, 128, y_block * plane_count)
    first_cos, first_sin = circle(blocks_x, blocks_x, blocks_x, -1.0)
    part_real, part_imag = contract(
        "fabm,aj->fmjb", columns[:field_total], columns[field_total:], first_cos, first_sin
    )
    twist_cos, twist_sin = circle(full_x, blocks_x, 128, -1.0)
    part_real, part_imag = rotate(part_real, part_imag, twist_cos, twist_sin)
    part_real, part_imag = contract("fmjb,bk->fmjk", part_real, part_imag, lane_cos, lane_sin)
    spectra_x = jnp.concatenate([part_real, part_imag], 0).reshape(
        2 * field_total, y_block, plane_count, full_x
    )
    depth_cos, depth_sin = circle(full_z, full_z, full_z, -1.0)
    own_cos = lax.dynamic_slice_in_dim(depth_cos, section_at * plane_count, plane_count, 0)
    own_sin = lax.dynamic_slice_in_dim(depth_sin, section_at * plane_count, plane_count, 0)
    term_real, term_imag = contract(
        "fyzk,zq->yfqk", spectra_x[:field_total], spectra_x[field_total:], own_cos, own_sin
    )
    spectral = lax.psum_scatter(
        jnp.concatenate([term_real, term_imag], 1), "section", scatter_dimension=0, tiled=True
    )
    storage_y = slab_at * y_block + section_at * y_half + jnp.arange(y_half, dtype=jnp.int32)
    storage_x = jnp.arange(full_x, dtype=jnp.int32)
    storage_z = jnp.arange(full_z, dtype=jnp.int32)
    wave_sq = (
        wave_square(storage_y, full_y, True)[:, None, None]
        + wave_square(storage_z, full_z, False)[None, :, None]
        + wave_square(storage_x, full_x, True)[None, None, :]
    )
    numerator = 1.0 + time_step * stabilizer * wave_sq
    denominator = numerator + time_step * kappa_grad * wave_sq * wave_sq
    keep_rate = numerator / denominator
    mix_rate = time_step * wave_sq / denominator
    new_real = keep_rate * spectral[:, 0] - mix_rate * spectral[:, 1]
    new_imag = keep_rate * spectral[:, 1] + mix_rate * spectral[:, 0]
    back_cos, back_sin = circle(full_z, full_z, full_z, 1.0)
    part_real, part_imag = contract("yqk,qz->yzk", new_real, new_imag, back_cos, back_sin)
    returning = jnp.stack([part_real, part_imag], 1)
    own_planes = lax.all_to_all(returning, "section", split_axis=2, concat_axis=0, tiled=True)
    grid_real = own_planes[:, 0].reshape(y_block, plane_count, blocks_x, 128)
    grid_imag = own_planes[:, 1].reshape(y_block, plane_count, blocks_x, 128)
    lane_cos, lane_sin = circle(128, 128, 128, 1.0)
    part_real, part_imag = contract("szjk,kb->szjb", grid_real, grid_imag, lane_cos, lane_sin)
    twist_cos, twist_sin = circle(full_x, blocks_x, 128, 1.0)
    part_real, part_imag = rotate(part_real, part_imag, twist_cos, twist_sin)
    first_cos, first_sin = circle(blocks_x, blocks_x, blocks_x, 1.0)
    part_real, part_imag = contract("szjb,ja->absz", part_real, part_imag, first_cos, first_sin)
    leaving = jnp.stack([part_real, part_imag], 0).reshape(2, full_x, 1, y_block * plane_count)
    rows_back = lax.all_to_all(leaving, "slab", split_axis=1, concat_axis=2, tiled=True)
    rows_back = rows_back.reshape(2, row_count, blocks_y, 128, plane_count)
    part_real, part_imag = contract("xjkz,kb->xjbz", rows_back[0], rows_back[1], lane_cos, lane_sin)
    twist_cos, twist_sin = circle(full_y, blocks_y, 128, 1.0)
    part_real, part_imag = rotate(
        part_real, part_imag, twist_cos[:, :, None], twist_sin[:, :, None]
    )
    first_cos, first_sin = circle(blocks_y, blocks_y, blocks_y, 1.0)
    new_field = real_only("xjbz,ja->zxab", part_real, part_imag, first_cos, first_sin)
    new_field = new_field.reshape(plane_count, row_count, full_y) / cell_count
    total_bulk = lax.psum(bulk_sum, ("section", "slab"))
    energy = total_bulk / cell_count
    return (new_field, energy)


lanes = 128
row_group = 32
groups = 8
kk = 8
vmem_limit = 48 * 1024 * 1024
small_limit = 8 * 1024 * 1024


def split(values):
    high = values.astype(jnp.bfloat16)
    low = (values - high.astype(jnp.float32)).astype(jnp.bfloat16)
    return high, low


def triple(left_parts, right_parts, dims):
    def product(left, right):
        return lax.dot_general(left, right, (dims, ((), ())), preferred_element_type=jnp.float32)

    left_high, left_low = left_parts
    right_high, right_low = right_parts
    return (
        product(left_high, right_high)
        + product(left_low, right_high)
        + product(left_high, right_low)
    )


def y_tables(full_y, devices, parity):
    half = full_y // 2
    per_part = half // 2 // devices
    slot = np.arange(half)
    device, inner = slot // (2 * per_part), slot % (2 * per_part)
    part, local = inner // per_part, inner % per_part
    wave = parity + 2 * (device * per_part + local)
    position = np.arange(half)
    turns = wave[:, None] * position[None, :] % full_y
    phase = turns * (2.0 * math.pi / full_y)
    coarse = phase[::row_group]
    offset = wave[:row_group] - wave[0]
    fine = (offset[:, None] * position[None, :] % full_y) * (2.0 * math.pi / full_y)
    fine = fine + part[:row_group, None] * (0.5 * math.pi)
    return [
        table.astype(np.float32)
        for table in (np.cos(coarse), np.sin(coarse), np.cos(fine), np.sin(fine))
    ]


def y_block(refs, block, parity, kk):
    coarse_cos, coarse_sin, fine_cos, fine_sin = refs
    cos_fine, sin_fine = fine_cos[...], fine_sin[...]
    pieces = []
    for inner in range(groups):
        at = pl.ds(block * groups + inner, 1)
        piece = coarse_cos[at, :] * cos_fine - coarse_sin[at, :] * sin_fine
        if parity == 0 and inner == 0:
            row = lax.broadcasted_iota(jnp.int32, piece.shape, 0)
            column = lax.broadcasted_iota(jnp.int32, piece.shape, 1)
            sign = 1.0 - 2.0 * (column % 2).astype(jnp.float32)
            wanted = jnp.where(block == 0, kk, -1)
            piece = jnp.where(row == wanted, sign, piece)
        pieces.append(piece)
    return jnp.concatenate(pieces, 0)


def times_unit(real, imag, quarter_turns):
    turns = quarter_turns % 4
    if turns == 0:
        return real, imag
    if turns == 1:
        return -imag, real
    if turns == 2:
        return -real, -imag
    return imag, -real


def unit_sum(parts, power, direction):
    total_real, total_imag = parts[0]
    for index in range(1, len(parts)):
        real, imag = times_unit(*parts[index], direction * power * index)
        total_real = total_real + real
        total_imag = total_imag + imag
    return total_real, total_imag


def flip(bit, wanted):
    return 1 - bit if wanted else bit


class Place:
    def __init__(self):
        self.section = lax.axis_index("section")
        self.slab = lax.axis_index("slab")
        self.upper = self.slab // 8
        depth = self.slab // 4 % 2
        self.inner = depth + self.upper - 2 * depth * self.upper
        self.bits = [self.slab % 2, self.slab // 2 % 2, 1 - self.inner, self.section]
        self.here = self.indices(self.bits)

    def indices(self, bits):
        inner = 1 - bits[2]
        depth = inner + self.upper - 2 * inner * self.upper
        low = bits[1] * 2 + bits[0]
        by_rows = bits[3] * 8 + depth * 4 + low
        by_waves = bits[3] * 8 + inner * 4 + low
        among_inner = bits[3] * 4 + low
        return by_rows, by_waves, among_inner, (bits[3], self.upper * 8 + depth * 4 + low)

    def peer(self, turn):
        return self.indices([flip(bit, turn >> at & 1) for at, bit in enumerate(self.bits)])

    def partner(self):
        return self.section, 12 - self.slab // 4 * 4 + self.slab % 4


def remote(source, target, send, receive, device):
    return pltpu.make_async_remote_copy(
        src_ref=source,
        dst_ref=target,
        send_sem=send,
        recv_sem=receive,
        device_id=device,
        device_id_type=pl.DeviceIdType.MESH,
    )


same_side = [8, 2, 10, 1, 9, 3, 11]
other_side = [4, 12, 6, 14, 5, 13, 7, 15]
turn_order = [4, 8, 6, 2, 12, 10, 5, 1, 14, 9, 13, 3, 7, 11, 15]
lead, lag, wait_lag = 4, 1, 6


def greet(place):
    barrier = pltpu.get_barrier_semaphore()
    devices = [place.peer(turn)[3] for turn in turn_order] + [place.partner()]
    for device in devices:
        pl.semaphore_signal(
            barrier, inc=1, device_id=device, device_id_type=pl.DeviceIdType.MESH
        )
    return lambda: pl.semaphore_wait(barrier, len(devices))


def step_kernel(cells, chunks, conc_from, y_from, x_from, *refs):
    even_ref, odd_ref, energy_ref = refs[0:3]
    (
        conc_ref, y_ref, x_ref, loaded,
        high_ref, low_ref, wide_high, wide_low, spec_ref, fil_ref,
        sent_ref, arrived_ref, own_ref, other_ref, partner_ref, returned_ref,
        tile_ref, half_ref, far_ref,
        sent_out, sent_in, other_out, other_in, own_out, own_in, tile_out, tile_in,
        half_out, half_in,
    ) = refs[3:]
    loads = [
        pltpu.make_async_copy(conc_from.at[0], conc_ref.at[0], loaded.at[0]),
        pltpu.make_async_copy(conc_from.at[1], conc_ref.at[1], loaded.at[4]),
        pltpu.make_async_copy(y_from.at[1], y_ref.at[1], loaded.at[1]),
        pltpu.make_async_copy(x_from, x_ref, loaded.at[2]),
        pltpu.make_async_copy(y_from.at[0], y_ref.at[0], loaded.at[3]),
    ]
    for load in loads:
        load.start()
    tables = [[y_ref.at[parity, at] for at in range(4)] for parity in range(2)]
    x_rows = x_ref.shape[0]
    short = row_group // 2
    starts = [0, 8, 16, 24, 24 + short, 24 + 2 * short, 24 + 2 * short + row_group]
    ends = starts[1:] + [x_rows]
    wx_ref, tw_cos, tw_sin, ca, sa, cb, sb = [
        x_ref.at[slice(start, end)] for start, end in zip(starts, ends)
    ]
    place = Place()
    by_rows, by_waves, among_inner, _ = place.here
    is_inner = place.inner == 1
    planes, rows, full_y = conc_ref.shape
    half = full_y // 2
    members, inner, columns = arrived_ref.shape[1:]
    items = arrived_ref.shape[0]
    width = spec_ref.shape[4]
    sections = 2
    full_z = planes * sections
    zf_local = planes * 2
    total_zf = zf_local * sections
    slabs = members // sections
    quarter = slabs // 2
    met = greet(place)

    def prepare(parity, wants_bulk, arriving=()):
        total = jnp.zeros((8, lanes), jnp.float32)
        for plane in range(planes):
            for load in arriving[plane : plane + 1]:
                load.wait()
            first = conc_ref[plane, :, :half]
            second = conc_ref[plane, :, half:]
            first_sq, second_sq = first * first, second * second
            if wants_bulk:
                bulk = 0.25 * (first_sq * first_sq + second_sq * second_sq)
                bulk = bulk - 0.5 * (first_sq + second_sq)
                bulk = jnp.sum(bulk.reshape(rows // 8, 8, half), axis=0)
                for at in range(0, half, lanes):
                    total = total + bulk[:, at : at + lanes]
            first_g = first_sq * first - first
            second_g = second_sq * second - second
            for field, (left, right) in enumerate(((first, second), (first_g, second_g))):
                mixed = left + right if parity == 0 else left - right
                high, low = split(mixed)
                at = (plane * 2 + field) * rows
                high_ref[at : at + rows, :] = high
                low_ref[at : at + rows, :] = low
        return total

    def forward(parity, sub, at):
        table = y_block(tables[parity], sub, parity, kk)
        result = triple(split(table), (high_ref[...], low_ref[...]), ((1,), (1,)))
        sent_ref[at] = result.reshape(members, inner, columns)

    def shared(item):
        return lax.rem(item, 3) == 0

    def takes(item):
        return shared(item) | is_inner

    def chunk_of(item):
        return item // 3 * 2 + jnp.where(shared(item), 0, 1)

    def slot_of(item, waves, order):
        return jnp.where(shared(item), waves, 2 * order + lax.rem(item, 3) - 1)

    def copies_out(item, turns):
        copies = []
        for turn in turns:
            _, waves, order, device = place.peer(turn)
            copies.append(
                remote(
                    sent_ref.at[chunk_of(item), slot_of(item, waves, order)],
                    arrived_ref.at[item, by_rows],
                    sent_out.at[item],
                    sent_in.at[item],
                    device,
                )
            )
        return copies

    def spread(item):
        @pl.when(shared(item))
        def _():
            start(copies_out(item, turn_order))

        @pl.when(~shared(item) & is_inner)
        def _():
            start(copies_out(item, same_side))

        @pl.when(~shared(item) & ~is_inner)
        def _():
            start(copies_out(item, other_side))

        @pl.when(takes(item))
        def _():
            slot = slot_of(item, by_waves, among_inner)
            arrived_ref[item, by_rows] = sent_ref[chunk_of(item), slot]

    def spread_tile():
        copies = []
        for turn in turn_order:
            copies.append(
                remote(
                    tile_ref.at[by_rows],
                    tile_ref.at[by_rows],
                    tile_out,
                    tile_in,
                    place.peer(turn)[3],
                )
            )
        return copies

    def wide_table():
        cos_rows, sin_rows = [], []
        cos_fine, sin_fine = cb[...], sb[...]
        for group in range(row_group // 2):
            cos_base, sin_base = ca[group : group + 1, :], sa[group : group + 1, :]
            cos_rows.append(cos_base * cos_fine - sin_base * sin_fine)
            sin_rows.append(sin_base * cos_fine + cos_base * sin_fine)
        table = jnp.concatenate([jnp.concatenate(cos_rows, 0), jnp.concatenate(sin_rows, 0)], 1)
        wide_high[...], wide_low[...] = split(table)

    def middle(item, has_extra):
        depth = 2 * kk if has_extra else kk
        chunk = chunk_of(item)
        sub = lax.rem(chunk, len(chunks) // 2)
        parity = jnp.where(chunk < len(chunks) // 2, 1, 0)
        slot = slot_of(item, by_waves, among_inner)
        base_wave = parity + 2 * kk * (sub * members + slot)
        row_iota = lax.broadcasted_iota(jnp.int32, (kk, 1), 0)
        special = None
        if has_extra:
            wanted = jnp.where(slot == 0, 0, -1)
            special = jnp.where(row_iota == wanted, 1.0, 0.0)

        def gather(section, a, part, zf):
            pieces = [
                arrived_ref[
                    item,
                    section * slabs + a * quarter + step,
                    part * kk : (part + 1) * kk,
                    zf * lanes : (zf + 1) * lanes,
                ]
                for step in range(quarter)
            ]
            return jnp.concatenate(pieces, 1)

        def put(parts, at, row):
            for j in range(4):
                real, imag = unit_sum(parts, j, -1)
                if j:
                    cos, sin = tw_cos[j : j + 1, :], tw_sin[j : j + 1, :]
                    real, imag = real * cos + imag * sin, imag * cos - real * sin
                spec_ref[j, 0, at, row : row + kk, :] = real
                spec_ref[j, 1, at, row : row + kk, :] = imag

        for section in range(sections):
            for zf in range(zf_local):
                at = section * zf_local + zf
                parts, extra = [], []
                for a in range(2):
                    real, imag = gather(section, a, 0, zf), gather(section, a, 1, zf)
                    if has_extra:
                        extra.append((imag * special, jnp.zeros_like(imag)))
                        imag = imag * (1.0 - special)
                    parts.append((real, imag))
                put(parts, at, 0)
                if has_extra:
                    put(extra, at, kk)

        weights = (wide_high[...], wide_low[...])

        def one(pair, carry):
            source = spec_ref[pl.ds(2 * pair, 2), :, :, 0:depth, :]
            raw = triple(split(source.reshape(4 * total_zf * depth, width)), weights, ((1,), (0,)))
            raw = raw.reshape(2, 2, total_zf, depth, 2 * width)
            for inside in range(2):
                j = 2 * pair + inside
                for row in range(0, depth, kk):
                    fields = []
                    for field in range(2):
                        per_z = []
                        for z in range(full_z):
                            re_part = raw[inside, 0, z * 2 + field, row : row + kk]
                            im_part = raw[inside, 1, z * 2 + field, row : row + kk]
                            per_z.append(
                                (
                                    re_part[:, :width] + im_part[:, width:],
                                    im_part[:, :width] - re_part[:, width:],
                                )
                            )
                        fields.append(per_z)
                    wave = base_wave + 2 * row_iota
                    if row:
                        wave = jnp.full_like(wave, half)
                    first = (wave == 0) | (wave == half)
                    weight = jnp.where(first, 1.0 / cells, 2.0 / cells)
                    angle = wave.astype(jnp.float32) * (2.0 * math.pi / full_y)
                    plane_sq = angle * angle + wx_ref[pl.ds(j, 1), :]
                    updated = []
                    for q in range(full_z):
                        c_real, c_imag = unit_sum(fields[0], q, -1)
                        g_real, g_imag = unit_sum(fields[1], q, -1)
                        signed = q - full_z if 2 * q >= full_z else q
                        wave_sq = plane_sq + (2.0 * math.pi * signed / full_z) ** 2
                        numerator = 1.0 + time_step * stabilizer * wave_sq
                        denominator = numerator + time_step * kappa_grad * wave_sq * wave_sq
                        inverse = weight / denominator
                        keep = numerator * inverse
                        mix = time_step * wave_sq * inverse
                        updated.append(
                            (keep * c_real - mix * g_real, keep * c_imag - mix * g_imag)
                        )
                    for z in range(full_z):
                        real, imag = unit_sum(updated, z, 1)
                        fil_ref[j, 0, z, row : row + kk, :] = real
                        fil_ref[j, 1, z, row : row + kk, :] = imag
            return carry

        lax.fori_loop(0, 2, one, 0)
        source = fil_ref[:, :, :, 0:depth, :].reshape(8 * full_z * depth, width)
        raw = triple(split(source), weights, ((1,), (0,))).reshape(4, 2, full_z, depth, 2 * width)

        def back(z, row):
            parts = []
            for j in range(4):
                re_part = raw[j, 0, z, row : row + kk]
                im_part = raw[j, 1, z, row : row + kk]
                real = re_part[:, :width] - im_part[:, width:]
                imag = re_part[:, width:] + im_part[:, :width]
                if j:
                    cos, sin = tw_cos[j : j + 1, :], tw_sin[j : j + 1, :]
                    real, imag = real * cos - imag * sin, imag * cos + real * sin
                parts.append((real, imag))
            return parts

        for z in range(full_z):
            section, plane = z // planes, z % planes
            parts = back(z, 0)
            extra = back(z, kk) if has_extra else None
            for a in range(4):
                real, imag = unit_sum(parts, a, 1)
                if has_extra:
                    extra_real, _ = unit_sum(extra, a, 1)
                    imag = imag * (1.0 - special) + extra_real * special
                target_ref = own_ref if a < 2 else other_ref
                for step in range(quarter):
                    target = section * slabs + a % 2 * quarter + step
                    piece = slice(step * lanes, (step + 1) * lanes)
                    at = plane * inner
                    target_ref[item, target, at : at + kk, :] = real[:, piece]
                    target_ref[item, target, at + kk : at + 2 * kk, :] = imag[:, piece]

    def cross(item):
        return remote(
            other_ref.at[item],
            partner_ref.at[item],
            other_out.at[item],
            other_in.at[item],
            place.partner(),
        )

    def far():
        return remote(half_ref, far_ref, half_out, half_in, place.partner())

    def join(item):
        @pl.when(takes(item))
        def _():
            cross(item).wait_recv()
            chunk, slot = chunk_of(item), slot_of(item, by_waves, among_inner)
            own_ref[item] = own_ref[item] + partner_ref[item]
            returned_ref[chunk, slot] = own_ref[item, by_rows]
            for turn in turn_order:
                rows_at, _, _, device = place.peer(turn)
                remote(
                    own_ref.at[item, rows_at],
                    returned_ref.at[chunk, slot],
                    own_out.at[item],
                    own_in.at[item],
                    device,
                ).start()

    def backward(parity, sub, chunk):
        turned = [
            returned_ref[chunk, :, plane * inner : (plane + 1) * inner, :]
            .reshape(members * inner, rows)
            .T
            for plane in range(planes)
        ]
        table = y_block(tables[parity], sub, parity, kk)
        term = triple(split(jnp.concatenate(turned, 0)), split(table), ((1,), (0,)))
        target = (even_ref, odd_ref)[parity]
        target[...] = target[...] + term

    def forth(item, count):
        return remote(
            sent_ref.at[0, 0:count],
            arrived_ref.at[item, 0:count],
            sent_out.at[item],
            sent_in.at[item],
            place.partner(),
        )

    def tile_all():
        part = tile_ref.at[0 : members - 1]
        return remote(part, part, tile_out, tile_in, place.partner())

    def home(item, count):
        return remote(
            own_ref.at[item, 0:count],
            returned_ref.at[chunk_of(item), 0:count],
            own_out.at[item],
            own_in.at[item],
            place.partner(),
        )

    def by_kind(item, act):
        for count, kind in (
            (members - 1, shared(item)),
            (len(same_side), ~shared(item) & is_inner),
            (len(other_side), ~shared(item) & ~is_inner),
        ):

            @pl.when(kind)
            def _():
                act(count)

    def wait_home(chunk):
        first = chunk // 2 * 3 + lax.rem(chunk, 2)
        by_kind(first, lambda count: home(first, count).wait_recv())

        @pl.when(lax.rem(chunk, 2) == 1)
        def _():
            by_kind(first + 1, lambda count: home(first + 1, count).wait_recv())

    def start(copies):
        for copy in copies:
            copy.start()

    total = len(chunks)
    subs = total // 2
    special_at = chunks.index((0, 0)) // 2 * 3
    even_ref[...] = jnp.zeros_like(even_ref)
    odd_ref[...] = jnp.zeros_like(odd_ref)
    prepare(1, False, loads)
    loads[2].wait()
    forward(1, 0, 0)
    met()
    spread(0)
    forward(1, 1, 1)
    loads[3].wait()
    wide_table()
    lax.fori_loop(2, subs, lambda at, carry: forward(1, at, at), None)
    spread(1)
    tile_ref[by_rows] = prepare(0, True)
    start(spread_tile())
    loads[4].wait()
    lax.fori_loop(0, subs, lambda at, carry: forward(0, at, subs + at), None)

    for item in range(2, lead):
        spread(item)

    def one(item, carry):
        @pl.when(takes(item))
        def _():
            forth(item, members - 1).wait_recv()

        @pl.when(item + lead < items)
        def _():
            spread(item + lead)

        @pl.when(takes(item))
        def _():
            @pl.when(item != special_at)
            def _():
                middle(item, False)

            @pl.when(item == special_at)
            def _():
                middle(item, True)

            cross(item).start()

        @pl.when(item == 0)
        def _():
            tile_all().wait_recv()
            half_ref[...] = jnp.sum(tile_ref[...], axis=0)
            far().start()

        @pl.when(item >= lag)
        def _():
            join(item - lag)

        @pl.when((item >= wait_lag) & (lax.rem(item, 3) != 1))
        def _():
            chunk = chunk_of(item - wait_lag)
            wait_home(chunk)
            backward(1, chunk, chunk)

        return carry

    lax.fori_loop(0, items, one, 0)
    far().wait_recv()
    energy_ref[0, 0] = jnp.sum(half_ref[...] + far_ref[...]) / cells

    def last(at, carry):
        @pl.when(at < lag)
        def _():
            join(at + items - lag)

        wait_home(at + subs)
        backward(0, at, at + subs)
        return carry

    lax.fori_loop(0, subs, last, 0)

    def sent(item, carry):
        by_kind(item, lambda count: forth(item, count).wait_send())

        @pl.when(takes(item))
        def _():
            home(item, members - 1).wait_send()
            cross(item).wait_send()

        return carry

    lax.fori_loop(0, items, sent, 0)
    tile_all().wait_send()
    far().wait_send()


def combine_kernel(even_ref, odd_ref, out_to, out_ref, stored):
    planes, rows, full_y = out_ref.shape
    half = full_y // 2
    step = rows // stored.shape[1]
    stores = []
    for plane in range(planes):
        for part in range(stored.shape[1]):
            here = slice(part * step, (part + 1) * step)
            at = slice(plane * rows + part * step, plane * rows + (part + 1) * step)
            even_rows, odd_rows = even_ref[at, :], odd_ref[at, :]
            out_ref[plane, here, :half] = even_rows + odd_rows
            out_ref[plane, here, half:] = even_rows - odd_rows
            store = pltpu.make_async_copy(
                out_ref.at[plane, here], out_to.at[plane, here], stored.at[plane, part]
            )
            store.start()
            stores.append(store)
    for store in stores:
        store.wait()


def kernel_step(concentration):
    planes, rows, full_y = concentration.shape
    slabs = lax.axis_size("slab")
    sections = lax.axis_size("section")
    members = slabs * sections // 2
    full_x = rows * slabs
    full_z = planes * sections
    cells = full_x * full_y * full_z
    half = full_y // 2
    subs = half // 2 // members // kk
    width = full_x // 4
    base = np.arange(width)
    step = 2.0 * math.pi / width
    coarse = base[::row_group, None] * base[None, :] % width * step
    fine = base[:row_group, None] * base[None, :] % width * step
    dft = [f(t).astype(np.float32) for t in (coarse, fine) for f in (np.cos, np.sin)]
    twist = np.arange(4)[:, None] * base[None, :] * (2.0 * math.pi / full_x)
    twist_cos, twist_sin = np.cos(twist).astype(np.float32), np.sin(twist).astype(np.float32)
    kx = np.arange(4)[:, None] + 4 * base[None, :]
    kx = np.where(2 * kx >= full_x, kx - full_x, kx) * (2.0 * math.pi / full_x)
    wave_x = (kx * kx).astype(np.float32)
    tables = [y_tables(full_y, members * subs, parity) for parity in range(2)]
    chunks = [(1, sub) for sub in range(subs)] + [(0, sub) for sub in range(subs)]
    count = len(chunks)
    items = count // 2 * 3
    columns = planes * 2 * rows
    y_rows = np.stack([np.stack(parts) for parts in tables])
    small = [np.concatenate([rows, rows]) for rows in (wave_x, twist_cos, twist_sin)]
    coarse_cos, coarse_sin, fine_cos, fine_sin = dft
    x_rows = np.concatenate([*small, coarse_cos, coarse_sin, fine_cos, fine_sin])
    operands = [concentration, y_rows, x_rows]
    f32, bf16 = jnp.float32, jnp.bfloat16
    vmem, dma = pltpu.VMEM, pltpu.SemaphoreType.DMA
    in_vmem = pl.BlockSpec(memory_space=pltpu.VMEM)
    half_back = vmem((items, members, 2 * kk * planes, rows), f32)
    even, odd, energy = pl.pallas_call(
        functools.partial(step_kernel, cells, chunks),
        out_shape=(
            jax.ShapeDtypeStruct((planes * rows, half), f32),
            jax.ShapeDtypeStruct((planes * rows, half), f32),
            jax.ShapeDtypeStruct((1, 1), f32),
        ),
        in_specs=[pl.BlockSpec(memory_space=pltpu.HBM)] * len(operands),
        out_specs=(in_vmem, in_vmem, pl.BlockSpec(memory_space=pltpu.SMEM)),
        scratch_shapes=[
            vmem(concentration.shape, f32),
            vmem(y_rows.shape, f32),
            vmem(x_rows.shape, f32),
            dma((5,)),
            vmem((columns, half), bf16),
            vmem((columns, half), bf16),
            vmem((width, 2 * width), bf16),
            vmem((width, 2 * width), bf16),
            vmem((4, 2, 2 * full_z, 2 * kk, width), f32),
            vmem((4, 2, full_z, 2 * kk, width), f32),
            vmem((count, members, 2 * kk, columns), f32),
            vmem((items, members, 2 * kk, columns), f32),
            half_back,
            half_back,
            half_back,
            vmem((count, members, 2 * kk * planes, rows), f32),
            vmem((members, 8, lanes), f32),
            vmem((8, lanes), f32),
            vmem((8, lanes), f32),
            *[dma((items,))] * 6,
            dma,
            dma,
            dma,
            dma,
        ],
        compiler_params=pltpu.CompilerParams(
            vmem_limit_bytes=vmem_limit, collective_id=0, has_side_effects=True
        ),
    )(*[pltpu.with_memory_space_constraint(jnp.asarray(x), pltpu.HBM) for x in operands])
    new_field = pl.pallas_call(
        combine_kernel,
        out_shape=jax.ShapeDtypeStruct(concentration.shape, f32),
        in_specs=[in_vmem] * 2,
        out_specs=pl.BlockSpec(memory_space=pltpu.HBM),
        scratch_shapes=[vmem(concentration.shape, f32), dma((planes, 4))],
        compiler_params=pltpu.CompilerParams(vmem_limit_bytes=small_limit),
    )(even, odd)
    return (new_field, energy.reshape(()))


def per_device(concentration):
    planes, rows, full_y = concentration.shape
    devices = lax.axis_size("slab") * lax.axis_size("section")
    share = full_y // 4 // devices
    fits = (
        rows == lanes
        and planes * lax.axis_size("section") == 4
        and share == 2 * kk
        and devices == 32
        and lax.axis_size("section") == 2
    )
    return kernel_step(concentration) if fits else plain_step(concentration)


def solution(mesh):
    return jax.shard_map(
        per_device,
        mesh=mesh,
        in_specs=(P("section", "slab", None),),
        out_specs=(P("section", "slab", None), P()),
        check_vma=False,
    )
```
